256 devices in a mesh: group: 2 (over y), pool: 2 (over core), slab: 64 (over z, x).
Axes of the slice: x: 4, y: 2, z: 16, core: 2. Of those that a mesh axis runs over, the one named last changes fastest.
The devices are a block of a 4x16x16 slice.
Arguments:
- drho_part: float32 [2, 32, 2, 128, 128, 128], P('pool', 'group', None, 'slab'), parts along dimension 1, may hold values from -6 to 6
- fxc: float32 [128, 128, 128], P('slab'), may hold values from -2 to -0.2
- cutoff_mask: int32 [128, 128, 128], P(None, 'slab'), may hold values 0 or 1
- owner_table: int32 [32], P('group'), parts along dimension 0, may hold values from 0 to 15, each once
Outputs:
- dv: float32 [32, 2, 128, 128, 128], P('group', None, 'slab'), parts along dimension 0
The draws below stay inside these ranges and needn't reach their ends.
There are 2 independent parts, one for each index of `group`. The reference program is written for one: setup_inputs(seed, part) draws one part's arguments, and reference() takes and returns one part's arrays. A program takes and returns all parts, laid end to end along the dimension named above; an argument that names none is the same for every part. Nothing has to cross between parts.
Inputs may be any that keep to these rules, and one draw needn't show every extreme that they name: `owner_table`: each perturbation appears in exactly one slot.
All inputs are finite; a program needn't handle non-finite values. No bound on the sum of `cutoff_mask` on one device may be relied on, other than what follows from the above.
Results may differ from the reference program's by a relative error of at most 0.00008.
Values sent between devices are 32-bit elements; how exact they have to be, the bound alone decides.
No kernel may reach another device: no remote copies, remote signals or barrier semaphores. Data moves between devices by JAX's collectives and lax.ppermute only.
A program may use at most 64 MiB of HBM per device.

```python
import math
import jax
import jax.numpy as jnp
from jax import lax

NG = 128
P_SIZE = 16
N_POOL = 2


def set_ends(array, rng, smallest, top_value):
    longest = array.shape.index(max(array.shape))
    spots = []
    for shift in (0, 1):
        where = [jax.random.randint(jax.random.fold_in(rng, axis), (), 0, length) for axis, length in enumerate(array.shape)]
        where[longest] = (where[longest] + shift) % array.shape[longest]
        spots.append(tuple(where))
    return array.at[spots[0]].set(smallest).at[spots[1]].set(top_value)


def shard_levels(stream_key, extent, cuts, low, top_value):
    level, own = 1.0, jax.random.fold_in(stream_key, 6)
    for position, shards_of in cuts:
        steps = jnp.exp(jax.random.uniform(jax.random.fold_in(own, position), (shards_of,), jnp.float32, low / len(cuts), top_value / len(cuts)))
        level = level * jnp.repeat(steps, extent[position] // shards_of).reshape([-1 if axis == position else 1 for axis in range(len(extent))])
    return level


def gaussian(stream_key, extent, width, reach, pieces=(), kind=jnp.bfloat16):
    drawn = jax.random.normal(stream_key, extent, jnp.float32) * width
    if len(pieces) > 0:
        drawn = shard_levels(stream_key, extent, pieces, -0.22, 0.18) * drawn
    return jnp.clip(drawn, min=-reach, max=reach).astype(kind)


def setup_inputs(seed: int = 0, part: int = 0) -> dict:
    key_of = jax.random.split(jax.random.key(seed), 5)
    own_keys = jax.random.split(jax.random.fold_in(key_of[4], part), 5)
    drho_part = gaussian(own_keys[0], (N_POOL, P_SIZE, 2, NG, NG, NG), 1.0, 6.0, ((0, 2), (3, 64)), jnp.float32)
    fxc = jnp.clip(-2.0 + 1.8 * jax.random.uniform(key_of[1], (NG, NG, NG), jnp.float32) ** shard_levels(key_of[1], (NG, NG, NG), ((0, 64),), -0.2, 0.2), -2.0, -0.2)
    cutoff_mask = set_ends((jax.random.randint(key_of[2], (NG, NG, NG), 0, 4) < 3).astype(jnp.int32), jax.random.fold_in(key_of[2], 1), 0, 1)
    owner_table = jax.random.permutation(own_keys[3], P_SIZE).astype(jnp.int32)
    return dict(drho_part=drho_part, fxc=fxc, cutoff_mask=cutoff_mask, owner_table=owner_table)


def kernel_table(cutoff_mask):
    index = jnp.arange(NG, dtype=jnp.int32)
    freq = ((index + NG // 2) % NG - NG // 2).astype(jnp.float32)
    square = freq * freq
    total = square[:, None, None] + square[None, :, None] + square[None, None, :]
    unit = (2.0 * math.pi / NG) ** 2
    return 4.0 * math.pi * cutoff_mask.astype(jnp.float32) / (unit * total + 0.25)


def reference(drho_part, fxc, cutoff_mask, owner_table):
    density = jnp.sum(drho_part, axis=0)
    ordered = jnp.take(density, owner_table, axis=0)
    kernel = kernel_table(cutoff_mask)

    def single(field):
        spectrum = jnp.fft.fftn(lax.complex(field[0], field[1]))
        hartree = jnp.fft.ifftn(spectrum * kernel)
        return jnp.stack([jnp.real(hartree) + fxc * field[0], jnp.imag(hartree) + fxc * field[1]])

    return lax.map(single, ordered)
```

```python
import functools
import math

import jax
import jax.numpy as jnp
import numpy as np
from jax import lax
from jax.experimental import pallas as pl
from jax.experimental.pallas import tpu as pltpu
from jax.sharding import PartitionSpec as P

F32 = jnp.float32
BF16 = jnp.bfloat16


def halves(table):
    high = table.astype(BF16)
    low = (table - high.astype(np.float64)).astype(BF16)
    return np.stack([high, low])


def dft(length, sign):
    index = np.arange(length)
    angle = 2.0 * np.pi * ((index[:, None] * index[None, :]) % length) / length
    cosine, sine = np.cos(angle), sign * np.sin(angle)
    return np.block([[cosine, -sine], [sine, cosine]])


def dealt_rows(length, devices, swap):
    width = length // devices
    rows = []
    for s in range(devices):
        s = s ^ 1 if swap else s
        rows += [r * length + s * width + b for r in range(2) for b in range(width)]
    return np.array(rows)


def dot3(left, right):
    dot = functools.partial(jnp.dot, preferred_element_type=F32)
    return dot(left[0], right[0]) + (dot(left[0], right[1]) + dot(left[1], right[0]))


def split(value):
    high = value.astype(BF16)
    return high, (value - high.astype(F32)).astype(BF16)


def send_kernel(owner, pool, local, out):
    out[...] = local[...]


def forward_kernel(owner, pool, first, second, arrived, wz, wy, *rest):
    spectrum, density = rest[-2:]
    n = first.shape[-1]
    mixed = []
    for k, local in enumerate((first, second)):
        x = local[0] + arrived[k]
        density[k] = x
        rows = jnp.concatenate([x[0].reshape(2 * n, n), x[1].reshape(2 * n, n)], axis=1)
        y = dot3(split(rows), (wz[0], wz[1]))
        real = jnp.concatenate([y[:n, :n], y[n:, :n]], axis=1)
        imag = jnp.concatenate([y[:n, n:], y[n:, n:]], axis=1)
        stacked = split(jnp.concatenate([real, imag], axis=0))
        mixed.append(dot3((wy[k, 0], wy[k, 1]), stacked).reshape(-1, 8, 2 * n))
    even, odd = mixed
    lower = lax.broadcasted_iota(jnp.int32, even.shape, 1) < 4
    for j, value in enumerate((jnp.where(lower, even, odd), jnp.where(lower, odd, even))):
        for a in range(2):
            spectrum[:, j, a, 0] = value[:, :, a * n : (a + 1) * n]


def middle_kernel(columns, wx, wxi, kernel, out, rows, back):
    n = kernel.shape[-1]
    length = kernel.shape[1]
    rows[...] = columns[...].reshape(rows.shape)
    grab = lambda j: rows[pl.ds(j, length, stride=8), :]
    order = [(p, b) for p in range(2) for b in range(2)]
    real = jnp.concatenate([grab(4 * p + b) for p, b in order], axis=1)
    imag = jnp.concatenate([grab(4 * p + 2 + b) for p, b in order], axis=1)
    spectrum = dot3((wx[0], wx[1]), split(jnp.concatenate([real, imag], axis=0)))
    both = jnp.concatenate([kernel[0], kernel[1]], axis=1)
    both = jnp.concatenate([both, both], axis=1)
    both = jnp.concatenate([both, both], axis=0)
    result = dot3((wxi[0], wxi[1]), split(spectrum * both))
    for i, (p, b) in enumerate(order):
        for r in range(2):
            back[pl.ds(4 * p + 2 * r + b, length, stride=8), :] = result[
                r * length : (r + 1) * length, i * n : (i + 1) * n
            ]
    out[...] = back[...].reshape(out.shape)


def backward_kernel(pool, columns, wyi, wzi, fxc, density, *rest):
    own, sent = rest[-2:]
    n = fxc.shape[-1]
    tiles = [jnp.concatenate([columns[:, j, a, 0] for a in range(2)], axis=-1) for j in range(2)]
    lower = lax.broadcasted_iota(jnp.int32, tiles[0].shape, 1) < 4
    even = jnp.where(lower, tiles[0], tiles[1])
    odd = jnp.where(lower, tiles[1], tiles[0])
    for k, value in enumerate((even, odd)):
        y = dot3((wyi[k, 0], wyi[k, 1]), split(value.reshape(2 * n, 2 * n)))
        rows = jnp.concatenate(
            [
                jnp.concatenate([y[:n, a * n : (a + 1) * n], y[n:, a * n : (a + 1) * n]], axis=1)
                for a in range(2)
            ],
            axis=0,
        )
        x = dot3(split(rows), (wzi[0], wzi[1]))
        for r in range(2):
            part = x[:, r * n : (r + 1) * n].reshape(2, n, n)
            value = part + fxc[...] * density[k, r]
            own[k, r] = value
            sent[k, r] = value


def place_kernel(pool, arrived, kept, out):
    out[...] = arrived[...]


def frequency(index, length):
    return ((index + length // 2) % length - length // 2).astype(F32)


def column_kernel(cutoff_mask, length):
    width = cutoff_mask.shape[1]
    start = lax.axis_index("slab") * width
    full_index = jnp.arange(length, dtype=jnp.int32)
    part_index = start + jnp.arange(width, dtype=jnp.int32)
    full_square = frequency(full_index, length) ** 2
    part_square = frequency(part_index, length) ** 2
    total = part_square[:, None, None] + full_square[None, :, None] + full_square[None, None, :]
    unit = (2.0 * math.pi / length) ** 2
    mask = jnp.swapaxes(cutoff_mask, 0, 1).astype(F32)
    scale = 1.0 / float(length) ** 3
    return (4.0 * math.pi * mask / (unit * total + 0.25)) * scale


def whole(array):
    return pl.BlockSpec(array.shape, lambda *_: (0,) * array.ndim)


def per_device(drho_part, fxc, cutoff_mask, owner_table):
    local = drho_part[0]
    slots, _, planes, n, _ = local.shape
    devices = lax.axis_size("slab")
    mine = slots // 2
    chunks = 2
    part = mine // chunks
    pairs = part // 2
    tile = (2, planes, n, n)
    pool = lax.axis_index("pool").astype(jnp.int32).reshape(1)
    swap = [(0, 1), (1, 0)]
    params = pltpu.CompilerParams(vmem_limit_bytes=40 << 20)

    forward = dft(n, -1.0)
    inverse = dft(n, 1.0)
    dealt = [dealt_rows(n, devices, s) for s in (False, True)]
    wz = jnp.asarray(halves(forward.T))
    wzi = jnp.asarray(halves(inverse.T))
    wy = jnp.asarray(np.stack([halves(forward[rows]) for rows in dealt]))
    wyi = jnp.asarray(np.stack([halves(inverse[:, rows]) for rows in dealt]))
    wx = jnp.asarray(halves(forward))
    wxi = jnp.asarray(halves(inverse))

    arrived = []
    for c in range(chunks):
        send = pl.pallas_call(
            send_kernel,
            out_shape=jax.ShapeDtypeStruct((part, *tile), F32),
            grid_spec=pltpu.PrefetchScalarGridSpec(
                num_scalar_prefetch=2,
                grid=(part,),
                in_specs=[
                    pl.BlockSpec((1, *tile), lambda i, own, q, c=c: (own[mine * (1 - q[0]) + part * c + i], 0, 0, 0, 0))
                ],
                out_specs=pl.BlockSpec((1, *tile), lambda i, own, q: (i, 0, 0, 0, 0)),
            ),
            compiler_params=params,
            name=f"send{c}",
        )(owner_table, pool, local)
        arrived.append(lax.ppermute(send, "pool", swap))

    shape = (devices // 2, 2, planes, mine // 2, 8, n)
    spectrum, densities = None, []
    for c in range(chunks):
        pick = lambda k, c=c: pl.BlockSpec(
            (1, *tile), lambda i, own, q: (own[mine * q[0] + part * c + 2 * i + k], 0, 0, 0, 0)
        )
        operands = [owner_table, pool, local, local, arrived[c], wz, wy]
        specs = [pick(0), pick(1), pl.BlockSpec((2, *tile), lambda i, own, q: (i, 0, 0, 0, 0)), whole(wz), whole(wy)]
        aliases = {}
        if spectrum is not None:
            aliases = {len(operands): 0}
            operands.append(spectrum)
            specs.append(pl.BlockSpec(memory_space=pl.ANY))
        spectrum, density = pl.pallas_call(
            forward_kernel,
            out_shape=(jax.ShapeDtypeStruct(shape, F32), jax.ShapeDtypeStruct((part, *tile), F32)),
            grid_spec=pltpu.PrefetchScalarGridSpec(
                num_scalar_prefetch=2,
                grid=(pairs,),
                in_specs=specs,
                out_specs=(
                    pl.BlockSpec(
                        (devices // 2, 2, planes, 1, 8, n), lambda i, own, q, c=c: (0, 0, 0, pairs * c + i, 0, 0)
                    ),
                    pl.BlockSpec((2, *tile), lambda i, own, q: (i, 0, 0, 0, 0)),
                ),
            ),
            input_output_aliases=aliases,
            compiler_params=params,
            name=f"forward{c}",
        )(*operands)
        densities.append(density)

    kernel = column_kernel(cutoff_mask, n)
    flat = (devices, planes * (mine // 2) * 8, n)
    columns = lax.all_to_all(spectrum.reshape(flat), "slab", split_axis=0, concat_axis=0, tiled=True)
    columns = columns.reshape(n, mine // 2, 8, n)
    block = pl.BlockSpec((n, 1, 8, n), lambda i: (0, i, 0, 0))
    columns = pl.pallas_call(
        middle_kernel,
        out_shape=jax.ShapeDtypeStruct(columns.shape, F32),
        grid=(mine // 2,),
        in_specs=[block, whole(wx), whole(wxi), whole(kernel)],
        out_specs=block,
        scratch_shapes=[pltpu.VMEM((n * 8, n), F32), pltpu.VMEM((n * 8, n), F32)],
        compiler_params=params,
        name="middle",
    )(columns, wx, wxi, kernel)
    columns = lax.all_to_all(columns.reshape(flat), "slab", split_axis=0, concat_axis=0, tiled=True)
    columns = columns.reshape(shape)

    out, others = None, []
    result = jax.ShapeDtypeStruct(local.shape, F32)
    for c in range(chunks):
        operands = [pool, columns, wyi, wzi, fxc, densities[c]]
        specs = [
            pl.BlockSpec((devices // 2, 2, planes, 1, 8, n), lambda i, q, c=c: (0, 0, 0, pairs * c + i, 0, 0)),
            whole(wyi),
            whole(wzi),
            whole(fxc),
            pl.BlockSpec((2, *tile), lambda i, q: (i, 0, 0, 0, 0)),
        ]
        aliases = {}
        if out is not None:
            aliases = {len(operands): 0}
            operands.append(out)
            specs.append(pl.BlockSpec(memory_space=pl.ANY))
        out, sent = pl.pallas_call(
            backward_kernel,
            out_shape=(result, jax.ShapeDtypeStruct((part, *tile), F32)),
            grid_spec=pltpu.PrefetchScalarGridSpec(
                num_scalar_prefetch=1,
                grid=(pairs,),
                in_specs=specs,
                out_specs=(
                    pl.BlockSpec((2, *tile), lambda i, q, c=c: (q[0] * (mine // 2) + pairs * c + i, 0, 0, 0, 0)),
                    pl.BlockSpec((2, *tile), lambda i, q: (i, 0, 0, 0, 0)),
                ),
            ),
            input_output_aliases=aliases,
            compiler_params=params,
            name=f"backward{c}",
        )(*operands)
        others.append(lax.ppermute(sent, "pool", swap))
    for c in range(chunks):
        out = pl.pallas_call(
            place_kernel,
            out_shape=result,
            grid_spec=pltpu.PrefetchScalarGridSpec(
                num_scalar_prefetch=1,
                grid=(pairs,),
                in_specs=[pl.BlockSpec((2, *tile), lambda i, q: (i, 0, 0, 0, 0)), pl.BlockSpec(memory_space=pl.ANY)],
                out_specs=pl.BlockSpec(
                    (2, *tile), lambda i, q, c=c: ((1 - q[0]) * (mine // 2) + pairs * c + i, 0, 0, 0, 0)
                ),
            ),
            input_output_aliases={2: 0},
            compiler_params=params,
            name=f"place{c}",
        )(pool, others[c], out)
    return out


def solution(mesh):
    placed = (
        P("pool", "group", None, "slab", None, None),
        P("slab", None, None),
        P(None, "slab", None),
        P("group"),
    )
    return jax.shard_map(
        per_device,
        mesh=mesh,
        in_specs=placed,
        out_specs=P("group", None, "slab", None, None),
        check_vma=False,
    )
```

```python
import functools
import math

import jax
import jax.numpy as jnp
import numpy as np
from jax import lax
from jax.experimental import pallas as pl
from jax.experimental.pallas import tpu as pltpu
from jax.sharding import PartitionSpec as P


F32 = jnp.float32
BF16 = jnp.bfloat16


def halves(table):
    high = table.astype(BF16)
    low = (table - high.astype(np.float64)).astype(BF16)
    return np.stack([high, low])


def dft(length, sign):
    index = np.arange(length)
    angle = 2.0 * np.pi * ((index[:, None] * index[None, :]) % length) / length
    cosine, sine = np.cos(angle), sign * np.sin(angle)
    return np.block([[cosine, -sine], [sine, cosine]])


def dealt_rows(length, devices, swap):
    width = length // devices
    rows = []
    for s in range(devices):
        s = s ^ 1 if swap else s
        rows += [r * length + s * width + b for r in range(2) for b in range(width)]
    return np.array(rows)


def dot3(left, right):
    dot = functools.partial(jnp.dot, preferred_element_type=F32)
    return dot(left[0], right[0]) + (dot(left[0], right[1]) + dot(left[1], right[0]))


def split(value):
    high = value.astype(BF16)
    return high, (value - high.astype(F32)).astype(BF16)


def gather(owner, start, local, kept, done, count):
    return [pltpu.make_async_copy(local.at[owner[start + k]], kept.at[k], done.at[k]) for k in range(count)]


def send_kernel(start, count, owner, pool, local, *rest):
    out, done = rest[-2:]
    copies = gather(owner, local.shape[0] // 2 * (1 - pool[0]) + start, local, out, done, count)
    for copy in copies:
        copy.start()
    for copy in copies:
        copy.wait()


def own_densities(start, count, owner, pool, local, kept, done):
    step = pl.program_id(0)
    copies = gather(owner, local.shape[0] // 2 * pool[0] + start, local, kept, done, count)

    @pl.when(step == 0)
    def _():
        for copy in copies:
            copy.start()

    for i in range(count // 2):

        @pl.when(step == i)
        def _():
            copies[2 * i].wait()
            copies[2 * i + 1].wait()


def forward_kernel(start, count, owner, pool, local, arrived, wz, wy, *rest):
    spectrum, kept, done = rest[-3:]
    n = kept.shape[-1]
    step = pl.program_id(0)
    own_densities(start, count, owner, pool, local, kept, done)
    mixed = []
    for k in range(2):
        x = kept[2 * step + k] + arrived[2 * step + k]
        rows = jnp.concatenate([x[0].reshape(2 * n, n), x[1].reshape(2 * n, n)], axis=1)
        y = dot3(split(rows), (wz[0], wz[1]))
        real = jnp.concatenate([y[:n, :n], y[n:, :n]], axis=1)
        imag = jnp.concatenate([y[:n, n:], y[n:, n:]], axis=1)
        stacked = split(jnp.concatenate([real, imag], axis=0))
        mixed.append(dot3((wy[k, 0], wy[k, 1]), stacked).reshape(-1, 8, 2 * n))
    even, odd = mixed
    lower = lax.broadcasted_iota(jnp.int32, even.shape, 1) < 4
    for j, value in enumerate((jnp.where(lower, even, odd), jnp.where(lower, odd, even))):
        for a in range(2):
            spectrum[:, j, a, 0] = value[:, :, a * n : (a + 1) * n]


def middle_kernel(columns, wx, wxi, kernel, out, rows, back):
    n = kernel.shape[-1]
    length = kernel.shape[1]
    step = pl.program_id(0)
    rows[...] = columns[:, step].reshape(rows.shape)
    grab = lambda j: rows[pl.ds(j, length, stride=8), :]
    order = [(p, b) for p in range(2) for b in range(2)]
    real = jnp.concatenate([grab(4 * p + b) for p, b in order], axis=1)
    imag = jnp.concatenate([grab(4 * p + 2 + b) for p, b in order], axis=1)
    spectrum = dot3((wx[0], wx[1]), split(jnp.concatenate([real, imag], axis=0)))
    both = jnp.concatenate([kernel[0], kernel[1]], axis=1)
    both = jnp.concatenate([both, both], axis=1)
    both = jnp.concatenate([both, both], axis=0)
    result = dot3((wxi[0], wxi[1]), split(spectrum * both))
    for i, (p, b) in enumerate(order):
        for r in range(2):
            back[pl.ds(4 * p + 2 * r + b, length, stride=8), :] = result[
                r * length : (r + 1) * length, i * n : (i + 1) * n
            ]
    out[:, step] = back[...].reshape(length, 8, n)


def backward_kernel(start, count, owner, pool, local, columns, wyi, wzi, fxc, arrived, *rest):
    own, sent, kept, done = rest[-4:]
    n = fxc.shape[-1]
    step = pl.program_id(0)
    own_densities(start, count, owner, pool, local, kept, done)
    place = start // 2 + step
    tiles = [jnp.concatenate([columns[:, j, a, place] for a in range(2)], axis=-1) for j in range(2)]
    lower = lax.broadcasted_iota(jnp.int32, tiles[0].shape, 1) < 4
    even = jnp.where(lower, tiles[0], tiles[1])
    odd = jnp.where(lower, tiles[1], tiles[0])
    for k, value in enumerate((even, odd)):
        y = dot3((wyi[k, 0], wyi[k, 1]), split(value.reshape(2 * n, 2 * n)))
        rows = jnp.concatenate(
            [
                jnp.concatenate([y[:n, a * n : (a + 1) * n], y[n:, a * n : (a + 1) * n]], axis=1)
                for a in range(2)
            ],
            axis=0,
        )
        x = dot3(split(rows), (wzi[0], wzi[1]))
        for r in range(2):
            part = x[:, r * n : (r + 1) * n].reshape(2, n, n)
            value = part + fxc[...] * (kept[2 * step + k, r] + arrived[2 * step + k, r])
            own[k, r] = value
            sent[2 * step + k, r] = value


def place_kernel(start, count, pool, arrived, kept, out, done):
    half = out.shape[0] // 2
    copy = pltpu.make_async_copy(arrived, out.at[pl.ds(half * (1 - pool[0]) + start, count)], done)
    copy.start()
    copy.wait()


def frequency(index, length):
    return ((index + length // 2) % length - length // 2).astype(F32)


def column_kernel(cutoff_mask, length):
    width = cutoff_mask.shape[1]
    start = lax.axis_index("slab") * width
    full_index = jnp.arange(length, dtype=jnp.int32)
    part_index = start + jnp.arange(width, dtype=jnp.int32)
    full_square = frequency(full_index, length) ** 2
    part_square = frequency(part_index, length) ** 2
    total = part_square[:, None, None] + full_square[None, :, None] + full_square[None, None, :]
    unit = (2.0 * math.pi / length) ** 2
    mask = jnp.swapaxes(cutoff_mask, 0, 1).astype(F32)
    scale = 1.0 / float(length) ** 3
    return (4.0 * math.pi * mask / (unit * total + 0.25)) * scale


RESIDENT = pl.BlockSpec(memory_space=pltpu.VMEM)


def taking(us):
    return pl.CostEstimate(flops=int(us * 1e8), bytes_accessed=0, transcendentals=0)


def per_device(drho_part, fxc, cutoff_mask, owner_table):
    local = drho_part[0]
    slots, _, planes, n, _ = local.shape
    devices = lax.axis_size("slab")
    mine = slots // 2
    tile = (2, planes, n, n)
    pool = lax.axis_index("pool").astype(jnp.int32).reshape(1)
    swap = [(0, 1), (1, 0)]
    limit = lambda share: pltpu.CompilerParams(vmem_limit_bytes=share << 20)
    ahead = [(0, 2), (2, mine - 2)]
    behind = ahead[::-1]

    forward = dft(n, -1.0)
    inverse = dft(n, 1.0)
    dealt = [dealt_rows(n, devices, s) for s in (False, True)]
    wz = jnp.asarray(halves(forward.T))
    wzi = jnp.asarray(halves(inverse.T))
    wy = jnp.asarray(np.stack([halves(forward[rows]) for rows in dealt]))
    wyi = jnp.asarray(np.stack([halves(inverse[:, rows]) for rows in dealt]))
    wx = jnp.asarray(halves(forward))
    wxi = jnp.asarray(halves(inverse))

    far = pl.BlockSpec(memory_space=pl.ANY)
    taken = lambda count: [pltpu.VMEM((count, *tile), F32), pltpu.SemaphoreType.DMA((count,))]

    arrived, sends = [], []
    for c, (start, count) in enumerate(ahead):
        sends.append(
            pl.pallas_call(
                functools.partial(send_kernel, start, count),
                out_shape=jax.ShapeDtypeStruct((count, *tile), F32),
                grid_spec=pltpu.PrefetchScalarGridSpec(
                    num_scalar_prefetch=2,
                    grid=(1,),
                    in_specs=[far] + [pl.BlockSpec(memory_space=pl.ANY)] * c,
                    out_specs=RESIDENT,
                    scratch_shapes=[pltpu.SemaphoreType.DMA((count,))],
                ),
                compiler_params=limit(54),
                cost_estimate=taking(0.7),
            )(owner_table, pool, local, *sends)
        )
        arrived.append(lax.ppermute(sends[-1], "pool", swap))

    shape = (devices // 2, 2, planes, mine // 2, 8, n)
    spectrum = None
    for c, (start, count) in enumerate(ahead):
        operands = [owner_table, pool, local, arrived[c], wz, wy]
        specs = [far, RESIDENT, RESIDENT, RESIDENT]
        aliases = {}
        if spectrum is not None:
            aliases = {len(operands): 0}
            operands.append(spectrum)
            specs.append(pl.BlockSpec(memory_space=pl.ANY))
        spectrum = pl.pallas_call(
            functools.partial(forward_kernel, start, count),
            out_shape=jax.ShapeDtypeStruct(shape, F32),
            grid_spec=pltpu.PrefetchScalarGridSpec(
                num_scalar_prefetch=2,
                grid=(count // 2,),
                in_specs=specs,
                out_specs=pl.BlockSpec(
                    (devices // 2, 2, planes, 1, 8, n), lambda i, *_, start=start: (0, 0, 0, start // 2 + i, 0, 0)
                ),
                scratch_shapes=taken(count),
            ),
            input_output_aliases=aliases,
            compiler_params=limit(40),
            cost_estimate=taking(0.8 * count),
        )(*operands)

    kernel = column_kernel(cutoff_mask, n)
    flat = (devices, planes * (mine // 2) * 8, n)
    columns = lax.all_to_all(spectrum.reshape(flat), "slab", split_axis=0, concat_axis=0, tiled=True)
    columns = columns.reshape(n, mine // 2, 8, n)
    columns = pl.pallas_call(
        middle_kernel,
        out_shape=jax.ShapeDtypeStruct(columns.shape, F32),
        grid=(mine // 2,),
        in_specs=[RESIDENT] * 4,
        out_specs=RESIDENT,
        scratch_shapes=[pltpu.VMEM((n * 8, n), F32), pltpu.VMEM((n * 8, n), F32)],
        compiler_params=limit(40),
        cost_estimate=taking(4),
        name="middle",
    )(columns, wx, wxi, kernel)
    columns = lax.all_to_all(columns.reshape(flat), "slab", split_axis=0, concat_axis=0, tiled=True)
    columns = columns.reshape(shape)

    out, others = None, []
    result = jax.ShapeDtypeStruct(local.shape, F32)
    for start, count in behind:
        operands = [owner_table, pool, local, columns, wyi, wzi, fxc, arrived[ahead.index((start, count))]]
        specs = [far] + [RESIDENT] * 5
        aliases = {}
        if out is not None:
            aliases = {len(operands): 0}
            operands.append(out)
            specs.append(pl.BlockSpec(memory_space=pl.ANY))
        out, sent = pl.pallas_call(
            functools.partial(backward_kernel, start, count),
            out_shape=(result, jax.ShapeDtypeStruct((count, *tile), F32)),
            grid_spec=pltpu.PrefetchScalarGridSpec(
                num_scalar_prefetch=2,
                grid=(count // 2,),
                in_specs=specs,
                out_specs=(
                    pl.BlockSpec(
                        (2, *tile), lambda i, own, q, start=start: (q[0] * (mine // 2) + start // 2 + i, 0, 0, 0, 0)
                    ),
                    RESIDENT,
                ),
                scratch_shapes=taken(count),
            ),
            input_output_aliases=aliases,
            compiler_params=limit(40),
            cost_estimate=taking(0.8 * count),
        )(*operands)
        others.append(lax.ppermute(sent, "pool", swap))
    for c, (start, count) in enumerate(behind):
        out = pl.pallas_call(
            functools.partial(place_kernel, start, count),
            out_shape=result,
            in_specs=[pl.BlockSpec(memory_space=pltpu.SMEM), RESIDENT, pl.BlockSpec(memory_space=pl.ANY)],
            out_specs=pl.BlockSpec(memory_space=pl.ANY),
            scratch_shapes=[pltpu.SemaphoreType.DMA],
            input_output_aliases={2: 0},
            compiler_params=limit(40),
            cost_estimate=taking(0.5),
        )(pool, others[c], out)
    return out


def solution(mesh):
    placed = (
        P("pool", "group", None, "slab", None, None),
        P("slab", None, None),
        P(None, "slab", None),
        P("group"),
    )

    return jax.shard_map(
        per_device,
        mesh=mesh,
        in_specs=placed,
        out_specs=P("group", None, "slab", None, None),
        check_vma=False,
    )
```

```python
import functools
import math

import jax
import jax.numpy as jnp
import numpy as np
from jax import lax
from jax.experimental import pallas as pl
from jax.experimental.pallas import tpu as pltpu
from jax.sharding import PartitionSpec as P


F32 = jnp.float32
BF16 = jnp.bfloat16


def halves(table):
    high = table.astype(BF16)
    low = (table - high.astype(np.float64)).astype(BF16)
    return np.stack([high, low])


def dft(length, sign):
    index = np.arange(length)
    angle = 2.0 * np.pi * ((index[:, None] * index[None, :]) % length) / length
    cosine, sine = np.cos(angle), sign * np.sin(angle)
    return np.block([[cosine, -sine], [sine, cosine]])


def dealt_rows(length, devices, swap):
    width = length // devices
    rows = []
    for s in range(devices):
        s = s ^ 1 if swap else s
        rows += [r * length + s * width + b for r in range(2) for b in range(width)]
    return np.array(rows)


def dot3(left, right):
    dot = functools.partial(jnp.dot, preferred_element_type=F32)
    return dot(left[0], right[0]) + (dot(left[0], right[1]) + dot(left[1], right[0]))


def split(value):
    high = value.astype(BF16)
    return high, (value - high.astype(F32)).astype(BF16)


def collect_kernel(start, count, pool, local, *rest):
    sent, own, done = rest[-3:]
    half = local.shape[0] // 2
    copies = [
        pltpu.make_async_copy(local.at[pl.ds(half * q + start, count)], kept, done.at[k])
        for k, (q, kept) in enumerate(((1 - pool[0], sent), (pool[0], own)))
    ]
    for copy in copies:
        copy.start()
    for copy in copies:
        copy.wait()


def forward_kernel(own, arrived, wz, wy, *rest):
    spectrum = rest[-1]
    n = own.shape[-1]
    step = pl.program_id(0)
    mixed = []
    for k in range(2):
        x = own[2 * step + k] + arrived[2 * step + k]
        rows = jnp.concatenate([x[0].reshape(2 * n, n), x[1].reshape(2 * n, n)], axis=1)
        y = dot3(split(rows), (wz[0], wz[1]))
        real = jnp.concatenate([y[:n, :n], y[n:, :n]], axis=1)
        imag = jnp.concatenate([y[:n, n:], y[n:, n:]], axis=1)
        stacked = split(jnp.concatenate([real, imag], axis=0))
        mixed.append(dot3((wy[k, 0], wy[k, 1]), stacked).reshape(-1, 8, 2 * n))
    even, odd = mixed
    lower = lax.broadcasted_iota(jnp.int32, even.shape, 1) < 4
    for j, value in enumerate((jnp.where(lower, even, odd), jnp.where(lower, odd, even))):
        for a in range(2):
            spectrum[:, j, a, 0] = value[:, :, a * n : (a + 1) * n]


def middle_kernel(columns, wx, wxi, kernel, out, rows, back):
    n = kernel.shape[-1]
    length = kernel.shape[1]
    step = pl.program_id(0)
    rows[...] = columns[:, step].reshape(rows.shape)
    grab = lambda j: rows[pl.ds(j, length, stride=8), :]
    order = [(p, b) for p in range(2) for b in range(2)]
    real = jnp.concatenate([grab(4 * p + b) for p, b in order], axis=1)
    imag = jnp.concatenate([grab(4 * p + 2 + b) for p, b in order], axis=1)
    spectrum = dot3((wx[0], wx[1]), split(jnp.concatenate([real, imag], axis=0)))
    both = jnp.concatenate([kernel[0], kernel[1]], axis=1)
    both = jnp.concatenate([both, both], axis=1)
    both = jnp.concatenate([both, both], axis=0)
    result = dot3((wxi[0], wxi[1]), split(spectrum * both))
    for i, (p, b) in enumerate(order):
        for r in range(2):
            back[pl.ds(4 * p + 2 * r + b, length, stride=8), :] = result[
                r * length : (r + 1) * length, i * n : (i + 1) * n
            ]
    out[:, step] = back[...].reshape(length, 8, n)


def backward_kernel(start, columns, wyi, wzi, fxc, own, arrived, out):
    n = fxc.shape[-1]
    step = pl.program_id(0)
    place = start // 2 + step
    tiles = [jnp.concatenate([columns[:, j, a, place] for a in range(2)], axis=-1) for j in range(2)]
    lower = lax.broadcasted_iota(jnp.int32, tiles[0].shape, 1) < 4
    even = jnp.where(lower, tiles[0], tiles[1])
    odd = jnp.where(lower, tiles[1], tiles[0])
    for k, value in enumerate((even, odd)):
        y = dot3((wyi[k, 0], wyi[k, 1]), split(value.reshape(2 * n, 2 * n)))
        rows = jnp.concatenate(
            [
                jnp.concatenate([y[:n, a * n : (a + 1) * n], y[n:, a * n : (a + 1) * n]], axis=1)
                for a in range(2)
            ],
            axis=0,
        )
        x = dot3(split(rows), (wzi[0], wzi[1]))
        for r in range(2):
            part = x[:, r * n : (r + 1) * n].reshape(2, n, n)
            out[2 * step + k, r] = part + fxc[...] * (own[2 * step + k, r] + arrived[2 * step + k, r])


def place_kernel(pieces, slot, pool, *rest):
    parts, out, done = rest[: len(pieces)], rest[-2], rest[-1]
    half = out.shape[0] // 2
    copies = []
    for (start, other), part in zip(pieces, parts):
        first = half * (1 - pool[0] if other else pool[0]) + start
        for k in range(part.shape[0]):
            copies.append(pltpu.make_async_copy(part.at[k], out.at[slot[first + k]], done.at[len(copies)]))
    for copy in copies:
        copy.start()
    for copy in copies:
        copy.wait()


def frequency(index, length):
    return ((index + length // 2) % length - length // 2).astype(F32)


def column_kernel(cutoff_mask, length):
    width = cutoff_mask.shape[1]
    start = lax.axis_index("slab") * width
    full_index = jnp.arange(length, dtype=jnp.int32)
    part_index = start + jnp.arange(width, dtype=jnp.int32)
    full_square = frequency(full_index, length) ** 2
    part_square = frequency(part_index, length) ** 2
    total = part_square[:, None, None] + full_square[None, :, None] + full_square[None, None, :]
    unit = (2.0 * math.pi / length) ** 2
    mask = jnp.swapaxes(cutoff_mask, 0, 1).astype(F32)
    scale = 1.0 / float(length) ** 3
    return (4.0 * math.pi * mask / (unit * total + 0.25)) * scale


RESIDENT = pl.BlockSpec(memory_space=pltpu.VMEM)


def taking(us):
    return pl.CostEstimate(flops=int(us * 1e8), bytes_accessed=0, transcendentals=0)


def per_device(drho_part, fxc, cutoff_mask, owner_table):
    local = drho_part[0]
    slots, _, planes, n, _ = local.shape
    devices = lax.axis_size("slab")
    mine = slots // 2
    tile = (2, planes, n, n)
    pool = lax.axis_index("pool").astype(jnp.int32).reshape(1)
    swap = [(0, 1), (1, 0)]
    limit = lambda share: pltpu.CompilerParams(vmem_limit_bytes=share << 20)
    ahead = [(0, 2), (2, mine - 2)]
    behind = ahead[::-1]

    forward = dft(n, -1.0)
    inverse = dft(n, 1.0)
    dealt = [dealt_rows(n, devices, s) for s in (False, True)]
    wz = jnp.asarray(halves(forward.T))
    wzi = jnp.asarray(halves(inverse.T))
    wy = jnp.asarray(np.stack([halves(forward[rows]) for rows in dealt]))
    wyi = jnp.asarray(np.stack([halves(inverse[:, rows]) for rows in dealt]))
    wx = jnp.asarray(halves(forward))
    wxi = jnp.asarray(halves(inverse))

    far = pl.BlockSpec(memory_space=pl.ANY)
    scalars = pl.BlockSpec(memory_space=pltpu.SMEM)
    parts = lambda count: jax.ShapeDtypeStruct((count, *tile), F32)

    own, arrived, sends = [], [], []
    for c, (start, count) in enumerate(ahead):
        sent, kept = pl.pallas_call(
            functools.partial(collect_kernel, start, count),
            out_shape=(parts(count), parts(count)),
            in_specs=[scalars, far] + [far] * c,
            out_specs=(RESIDENT, RESIDENT),
            scratch_shapes=[pltpu.SemaphoreType.DMA((2,))],
            compiler_params=limit(52 if c == 0 else 49),
            cost_estimate=taking(1),
        )(pool, local, *sends)
        sends.append(sent)
        own.append(kept)
        arrived.append(lax.ppermute(sent, "pool", swap))

    shape = (devices // 2, 2, planes, mine // 2, 8, n)
    spectrum = None
    for c, (start, count) in enumerate(ahead):
        operands = [own[c], arrived[c], wz, wy]
        specs = [RESIDENT] * 4
        aliases = {}
        if spectrum is not None:
            aliases = {len(operands): 0}
            operands.append(spectrum)
            specs.append(far)
        spectrum = pl.pallas_call(
            forward_kernel,
            out_shape=jax.ShapeDtypeStruct(shape, F32),
            grid=(count // 2,),
            in_specs=specs,
            out_specs=pl.BlockSpec(
                (devices // 2, 2, planes, 1, 8, n), lambda i, start=start: (0, 0, 0, start // 2 + i, 0, 0)
            ),
            input_output_aliases=aliases,
            compiler_params=limit(40),
            cost_estimate=taking(0.6 * count),
        )(*operands)

    kernel = column_kernel(cutoff_mask, n)
    index = jnp.arange(slots, dtype=jnp.int32)
    slot = jnp.sum(jnp.where(owner_table[None, :] == index[:, None], index[None, :], 0), axis=1)
    flat = (devices, planes * (mine // 2) * 8, n)
    columns = lax.all_to_all(spectrum.reshape(flat), "slab", split_axis=0, concat_axis=0, tiled=True)
    columns = columns.reshape(n, mine // 2, 8, n)
    columns = pl.pallas_call(
        middle_kernel,
        out_shape=jax.ShapeDtypeStruct(columns.shape, F32),
        grid=(mine // 2,),
        in_specs=[RESIDENT] * 4,
        out_specs=RESIDENT,
        scratch_shapes=[pltpu.VMEM((n * 8, n), F32), pltpu.VMEM((n * 8, n), F32)],
        compiler_params=limit(40),
        cost_estimate=taking(4),
        name="middle",
    )(columns, wx, wxi, kernel)
    columns = lax.all_to_all(columns.reshape(flat), "slab", split_axis=0, concat_axis=0, tiled=True)
    columns = columns.reshape(shape)

    results, others = [], []
    for start, count in behind:
        k = ahead.index((start, count))
        results.append(
            pl.pallas_call(
                functools.partial(backward_kernel, start),
                out_shape=parts(count),
                grid=(count // 2,),
                in_specs=[RESIDENT] * 6,
                out_specs=RESIDENT,
                compiler_params=limit(40),
                cost_estimate=taking(0.6 * count),
            )(columns, wyi, wzi, fxc, own[k], arrived[k])
        )
        others.append(lax.ppermute(results[-1], "pool", swap))

    def placed(pieces, arrays, out=None):
        aliases = {} if out is None else {2 + len(arrays): 0}
        kept = [] if out is None else [out]
        return pl.pallas_call(
            functools.partial(place_kernel, pieces),
            out_shape=jax.ShapeDtypeStruct(local.shape, F32),
            in_specs=[scalars, scalars] + [RESIDENT] * len(arrays) + [far] * len(kept),
            out_specs=far,
            scratch_shapes=[pltpu.SemaphoreType.DMA((sum(a.shape[0] for a in arrays),))],
            input_output_aliases=aliases,
            compiler_params=limit(40),
            cost_estimate=taking(1),
        )(slot, pool, *arrays, *kept)

    starts = [start for start, _ in behind]
    out = placed([(starts[0], False), (starts[1], False), (starts[0], True)], [*results, others[0]])
    return placed([(starts[1], True)], [others[1]], out)


def solution(mesh):
    placed = (
        P("pool", "group", None, "slab", None, None),
        P("slab", None, None),
        P(None, "slab", None),
        P("group"),
    )

    return jax.shard_map(
        per_device,
        mesh=mesh,
        in_specs=placed,
        out_specs=P("group", None, "slab", None, None),
        check_vma=False,
    )
```

```python
import functools
import math

import jax
import jax.numpy as jnp
import numpy as np
from jax import lax
from jax.experimental import pallas as pl
from jax.experimental.pallas import tpu as pltpu
from jax.sharding import PartitionSpec as P


F32 = jnp.float32
BF16 = jnp.bfloat16


def halves(table):
    high = table.astype(BF16)
    low = (table - high.astype(np.float64)).astype(BF16)
    return np.stack([high, low])


def dft(length, sign):
    index = np.arange(length)
    angle = 2.0 * np.pi * ((index[:, None] * index[None, :]) % length) / length
    cosine, sine = np.cos(angle), sign * np.sin(angle)
    return np.block([[cosine, -sine], [sine, cosine]])


def dealt_rows(length, devices, swap):
    width = length // devices
    rows = []
    for s in range(devices):
        s = s ^ 1 if swap else s
        rows += [r * length + s * width + b for r in range(2) for b in range(width)]
    return np.array(rows)


def dot3(left, right):
    dot = functools.partial(jnp.dot, preferred_element_type=F32)
    return dot(left[0], right[0]) + (dot(left[0], right[1]) + dot(left[1], right[0]))


def split(value):
    high = value.astype(BF16)
    return high, (value - high.astype(F32)).astype(BF16)


def collect_kernel(parts, other, pool, local, *rest):
    kept, done = rest[-1 - len(parts) : -1], rest[-1]
    first = local.shape[0] // 2 * (1 - pool[0] if other else pool[0])
    copies = [
        pltpu.make_async_copy(local.at[pl.ds(first + start, count)], part, done.at[k])
        for k, ((start, count), part) in enumerate(zip(parts, kept))
    ]
    for copy in copies:
        copy.start()
    for copy in copies:
        copy.wait()


def forward_kernel(own, arrived, wz, wy, *rest):
    spectrum = rest[-1]
    n = own.shape[-1]
    step = pl.program_id(0)
    mixed = []
    for k in range(2):
        x = own[2 * step + k] + arrived[2 * step + k]
        rows = jnp.concatenate([x[0].reshape(2 * n, n), x[1].reshape(2 * n, n)], axis=1)
        y = dot3(split(rows), (wz[0], wz[1]))
        real = jnp.concatenate([y[:n, :n], y[n:, :n]], axis=1)
        imag = jnp.concatenate([y[:n, n:], y[n:, n:]], axis=1)
        stacked = split(jnp.concatenate([real, imag], axis=0))
        mixed.append(dot3((wy[k, 0], wy[k, 1]), stacked).reshape(-1, 8, 2 * n))
    even, odd = mixed
    lower = lax.broadcasted_iota(jnp.int32, even.shape, 1) < 4
    for j, value in enumerate((jnp.where(lower, even, odd), jnp.where(lower, odd, even))):
        for a in range(2):
            spectrum[:, j, a, 0] = value[:, :, a * n : (a + 1) * n]


def middle_kernel(columns, wx, wxi, kernel, out, rows, back):
    n = kernel.shape[-1]
    length = kernel.shape[1]
    step = pl.program_id(0)
    rows[...] = columns[:, step].reshape(rows.shape)
    grab = lambda j: rows[pl.ds(j, length, stride=8), :]
    order = [(p, b) for p in range(2) for b in range(2)]
    real = jnp.concatenate([grab(4 * p + b) for p, b in order], axis=1)
    imag = jnp.concatenate([grab(4 * p + 2 + b) for p, b in order], axis=1)
    spectrum = dot3((wx[0], wx[1]), split(jnp.concatenate([real, imag], axis=0)))
    both = jnp.concatenate([kernel[0], kernel[1]], axis=1)
    both = jnp.concatenate([both, both], axis=1)
    both = jnp.concatenate([both, both], axis=0)
    result = dot3((wxi[0], wxi[1]), split(spectrum * both))
    for i, (p, b) in enumerate(order):
        for r in range(2):
            back[pl.ds(4 * p + 2 * r + b, length, stride=8), :] = result[
                r * length : (r + 1) * length, i * n : (i + 1) * n
            ]
    out[:, step] = back[...].reshape(length, 8, n)


def backward_kernel(start, columns, wyi, wzi, fxc, own, arrived, out):
    n = fxc.shape[-1]
    step = pl.program_id(0)
    place = start // 2 + step
    tiles = [jnp.concatenate([columns[:, j, a, place] for a in range(2)], axis=-1) for j in range(2)]
    lower = lax.broadcasted_iota(jnp.int32, tiles[0].shape, 1) < 4
    even = jnp.where(lower, tiles[0], tiles[1])
    odd = jnp.where(lower, tiles[1], tiles[0])
    for k, value in enumerate((even, odd)):
        y = dot3((wyi[k, 0], wyi[k, 1]), split(value.reshape(2 * n, 2 * n)))
        rows = jnp.concatenate(
            [
                jnp.concatenate([y[:n, a * n : (a + 1) * n], y[n:, a * n : (a + 1) * n]], axis=1)
                for a in range(2)
            ],
            axis=0,
        )
        x = dot3(split(rows), (wzi[0], wzi[1]))
        for r in range(2):
            part = x[:, r * n : (r + 1) * n].reshape(2, n, n)
            out[2 * step + k, r] = part + fxc[...] * (own[2 * step + k, r] + arrived[2 * step + k, r])


def place_kernel(pieces, slot, pool, *rest):
    parts, out, done = rest[: len(pieces)], rest[-2], rest[-1]
    half = out.shape[0] // 2
    copies = []
    for (start, other), part in zip(pieces, parts):
        first = half * (1 - pool[0] if other else pool[0]) + start
        for k in range(part.shape[0]):
            copies.append(pltpu.make_async_copy(part.at[k], out.at[slot[first + k]], done.at[len(copies)]))
    for copy in copies:
        copy.start()
    for copy in copies:
        copy.wait()


def frequency(index, length):
    return ((index + length // 2) % length - length // 2).astype(F32)


def column_kernel(cutoff_mask, length):
    width = cutoff_mask.shape[1]
    start = lax.axis_index("slab") * width
    full_index = jnp.arange(length, dtype=jnp.int32)
    part_index = start + jnp.arange(width, dtype=jnp.int32)
    full_square = frequency(full_index, length) ** 2
    part_square = frequency(part_index, length) ** 2
    total = part_square[:, None, None] + full_square[None, :, None] + full_square[None, None, :]
    unit = (2.0 * math.pi / length) ** 2
    mask = jnp.swapaxes(cutoff_mask, 0, 1).astype(F32)
    scale = 1.0 / float(length) ** 3
    return (4.0 * math.pi * mask / (unit * total + 0.25)) * scale


RESIDENT = pl.BlockSpec(memory_space=pltpu.VMEM)


def taking(us):
    return pl.CostEstimate(flops=int(us * 1e8), bytes_accessed=0, transcendentals=0)


def per_device(drho_part, fxc, cutoff_mask, owner_table):
    local = drho_part[0]
    slots, _, planes, n, _ = local.shape
    devices = lax.axis_size("slab")
    mine = slots // 2
    tile = (2, planes, n, n)
    pool = lax.axis_index("pool").astype(jnp.int32).reshape(1)
    swap = [(0, 1), (1, 0)]
    limit = lambda share: pltpu.CompilerParams(vmem_limit_bytes=share << 20)
    ahead = [(0, mine // 2), (mine // 2, mine // 2)]
    behind = ahead

    forward = dft(n, -1.0)
    inverse = dft(n, 1.0)
    dealt = [dealt_rows(n, devices, s) for s in (False, True)]
    wz = jnp.asarray(halves(forward.T))
    wzi = jnp.asarray(halves(inverse.T))
    wy = jnp.asarray(np.stack([halves(forward[rows]) for rows in dealt]))
    wyi = jnp.asarray(np.stack([halves(inverse[:, rows]) for rows in dealt]))
    wx = jnp.asarray(halves(forward))
    wxi = jnp.asarray(halves(inverse))

    far = pl.BlockSpec(memory_space=pl.ANY)
    scalars = pl.BlockSpec(memory_space=pltpu.SMEM)
    parts = lambda count: jax.ShapeDtypeStruct((count, *tile), F32)

    def collected(other, share):
        return pl.pallas_call(
            functools.partial(collect_kernel, ahead, other),
            out_shape=tuple(parts(count) for _, count in ahead),
            in_specs=[scalars, far],
            out_specs=(RESIDENT,) * len(ahead),
            scratch_shapes=[pltpu.SemaphoreType.DMA((len(ahead),))],
            compiler_params=limit(share),
            cost_estimate=taking(1),
        )(pool, local)

    arrived = []
    for sent in collected(True, 49):
        arrived.append(lax.ppermute(sent, "pool", swap))
    own = collected(False, 49)

    shape = (devices // 2, 2, planes, mine // 2, 8, n)
    spectrum = None
    for c, (start, count) in enumerate(ahead):
        operands = [own[c], arrived[c], wz, wy]
        specs = [RESIDENT] * 4
        aliases = {}
        if spectrum is not None:
            aliases = {len(operands): 0}
            operands.append(spectrum)
            specs.append(far)
        spectrum = pl.pallas_call(
            forward_kernel,
            out_shape=jax.ShapeDtypeStruct(shape, F32),
            grid=(count // 2,),
            in_specs=specs,
            out_specs=pl.BlockSpec(
                (devices // 2, 2, planes, 1, 8, n), lambda i, start=start: (0, 0, 0, start // 2 + i, 0, 0)
            ),
            input_output_aliases=aliases,
            compiler_params=limit(40),
            cost_estimate=taking(0.6 * count),
        )(*operands)

    kernel = column_kernel(cutoff_mask, n)
    index = jnp.arange(slots, dtype=jnp.int32)
    slot = jnp.sum(jnp.where(owner_table[None, :] == index[:, None], index[None, :], 0), axis=1)
    flat = (devices, planes * (mine // 2) * 8, n)
    columns = lax.all_to_all(spectrum.reshape(flat), "slab", split_axis=0, concat_axis=0, tiled=True)
    columns = columns.reshape(n, mine // 2, 8, n)
    columns = pl.pallas_call(
        middle_kernel,
        out_shape=jax.ShapeDtypeStruct(columns.shape, F32),
        grid=(mine // 2,),
        in_specs=[RESIDENT] * 4,
        out_specs=RESIDENT,
        scratch_shapes=[pltpu.VMEM((n * 8, n), F32), pltpu.VMEM((n * 8, n), F32)],
        compiler_params=limit(40),
        cost_estimate=taking(4),
        name="middle",
    )(columns, wx, wxi, kernel)
    columns = lax.all_to_all(columns.reshape(flat), "slab", split_axis=0, concat_axis=0, tiled=True)
    columns = columns.reshape(shape)

    results, others = [], []
    for start, count in behind:
        k = ahead.index((start, count))
        results.append(
            pl.pallas_call(
                functools.partial(backward_kernel, start),
                out_shape=parts(count),
                grid=(count // 2,),
                in_specs=[RESIDENT] * 6,
                out_specs=RESIDENT,
                compiler_params=limit(40),
                cost_estimate=taking(0.6 * count),
            )(columns, wyi, wzi, fxc, own[k], arrived[k])
        )
        others.append(lax.ppermute(results[-1], "pool", swap))

    def placed(pieces, arrays, out=None):
        aliases = {} if out is None else {2 + len(arrays): 0}
        kept = [] if out is None else [out]
        return pl.pallas_call(
            functools.partial(place_kernel, pieces),
            out_shape=jax.ShapeDtypeStruct(local.shape, F32),
            in_specs=[scalars, scalars] + [RESIDENT] * len(arrays) + [far] * len(kept),
            out_specs=far,
            scratch_shapes=[pltpu.SemaphoreType.DMA((sum(a.shape[0] for a in arrays),))],
            input_output_aliases=aliases,
            compiler_params=limit(40),
            cost_estimate=taking(1),
        )(slot, pool, *arrays, *kept)

    starts = [start for start, _ in behind]
    out = placed([(starts[0], False), (starts[1], False), (starts[0], True)], [*results, others[0]])
    return placed([(starts[1], True)], [others[1]], out)


def solution(mesh):
    placed = (
        P("pool", "group", None, "slab", None, None),
        P("slab", None, None),
        P(None, "slab", None),
        P("group"),
    )

    return jax.shard_map(
        per_device,
        mesh=mesh,
        in_specs=placed,
        out_specs=P("group", None, "slab", None, None),
        check_vma=False,
    )
```

```python
import functools
import math

import jax
import jax.numpy as jnp
import numpy as np
from jax import lax
from jax.experimental import pallas as pl
from jax.experimental.pallas import tpu as pltpu
from jax.sharding import PartitionSpec as P


F32 = jnp.float32
BF16 = jnp.bfloat16


def halves(table):
    high = table.astype(BF16)
    low = (table - high.astype(np.float64)).astype(BF16)
    return np.stack([high, low])


def dft(length, sign):
    index = np.arange(length)
    angle = 2.0 * np.pi * ((index[:, None] * index[None, :]) % length) / length
    cosine, sine = np.cos(angle), sign * np.sin(angle)
    return np.block([[cosine, -sine], [sine, cosine]])


def dft_halves(length, sign):
    outputs = np.arange(length).reshape(-1, 2).T
    parts = []
    for k in outputs:
        angle = 2.0 * np.pi * ((k[:, None] * np.arange(length // 2)[None, :]) % length) / length
        cosine, sine = np.cos(angle), sign * np.sin(angle)
        parts.append(np.block([[cosine, -sine], [sine, cosine]]))
    return parts


def dealt_rows(length, devices, swap):
    width = length // devices
    rows = []
    for s in range(devices):
        s = s ^ 1 if swap else s
        rows += [r * length + s * width + b for r in range(2) for b in range(width)]
    return np.array(rows)


def dot3(left, right):
    dot = functools.partial(jnp.dot, preferred_element_type=F32)
    return dot(left[0], right[0]) + (dot(left[0], right[1]) + dot(left[1], right[0]))


def split(value):
    high = value.astype(BF16)
    return high, (value - high.astype(F32)).astype(BF16)


def collect_kernel(parts, other, local, *rest):
    kept, done = rest[-1 - len(parts) : -1], rest[-1]
    pool = lax.axis_index("pool")
    first = local.shape[0] // 2 * (1 - pool if other else pool)
    copies = [
        pltpu.make_async_copy(local.at[pl.ds(first + start, count)], part, done.at[k])
        for k, ((start, count), part) in enumerate(zip(parts, kept))
    ]
    for copy in copies:
        copy.start()
    for copy in copies:
        copy.wait()


def forward_kernel(own, arrived, wz, wy, *rest):
    spectrum = rest[-1]
    n = own.shape[-1]
    step = pl.program_id(0)
    mixed = []
    for k in range(2):
        x = own[2 * step + k] + arrived[2 * step + k]
        rows = jnp.concatenate([x[0].reshape(2 * n, n), x[1].reshape(2 * n, n)], axis=1)
        y = dot3(split(rows), (wz[0], wz[1]))
        real = jnp.concatenate([y[:n, :n], y[n:, :n]], axis=1)
        imag = jnp.concatenate([y[:n, n:], y[n:, n:]], axis=1)
        stacked = split(jnp.concatenate([real, imag], axis=0))
        mixed.append(dot3((wy[k, 0], wy[k, 1]), stacked).reshape(-1, 8, 2 * n))
    even, odd = mixed
    lower = lax.broadcasted_iota(jnp.int32, even.shape, 1) < 4
    for j, value in enumerate((jnp.where(lower, even, odd), jnp.where(lower, odd, even))):
        for a in range(2):
            spectrum[:, j, a, 0] = value[:, :, a * n : (a + 1) * n]


def by_parts(table, even, odd):
    dot = functools.partial(jnp.dot, preferred_element_type=F32)
    (even_high, even_low), (odd_high, odd_low) = split(even), split(odd)
    main = [
        dot(jnp.concatenate([table[i, 0], table[i, 0]], axis=1), jnp.concatenate([high, low], axis=0))
        for i, (high, low) in enumerate(((even_high, even_low), (odd_high, odd_low)))
    ]
    zero = jnp.zeros(table.shape[2:], BF16)
    low = jnp.concatenate(
        [jnp.concatenate([table[0, 1], zero], axis=1), jnp.concatenate([zero, table[1, 1]], axis=1)], axis=0
    )
    return jnp.concatenate(main, axis=0) + dot(low, jnp.concatenate([even_high, odd_high], axis=0))


def middle_kernel(columns, wx, wxi, kernel, out, rows, back):
    n = kernel.shape[-1]
    length = kernel.shape[1]
    half = length // 2
    step = pl.program_id(0)
    rows[...] = columns[:, step].reshape(rows.shape)
    grab = lambda j: rows[pl.ds(j, length, stride=8), :]
    order = [(p, b) for p in range(2) for b in range(2)]
    fields = [jnp.concatenate([grab(4 * p + 2 * r + b) for p, b in order], axis=1) for r in range(2)]
    total = jnp.concatenate([f[:half] + f[half:] for f in fields], axis=0)
    difference = jnp.concatenate([f[:half] - f[half:] for f in fields], axis=0)
    spectrum = by_parts(wx, total, difference)
    both = jnp.concatenate([kernel[0], kernel[1]] * 2, axis=1)
    both = jnp.concatenate([both[:half], both[:half], both[half:], both[half:]], axis=0)
    spectrum = spectrum * both
    result = by_parts(wxi, spectrum[:length], spectrum[length:])
    even, odd = result[:length], result[length:]
    sides = (even + odd, even - odd)
    for i, (p, b) in enumerate(order):
        for r in range(2):
            for h, side in enumerate(sides):
                back[pl.ds(h * half * 8 + 4 * p + 2 * r + b, half, stride=8), :] = side[
                    r * half : (r + 1) * half, i * n : (i + 1) * n
                ]
    out[:, step] = back[...].reshape(length, 8, n)


def backward_kernel(start, columns, wyi, wzi, fxc, own, arrived, out):
    n = fxc.shape[-1]
    step = pl.program_id(0)
    place = start // 2 + step
    tiles = [jnp.concatenate([columns[:, j, a, place] for a in range(2)], axis=-1) for j in range(2)]
    lower = lax.broadcasted_iota(jnp.int32, tiles[0].shape, 1) < 4
    even = jnp.where(lower, tiles[0], tiles[1])
    odd = jnp.where(lower, tiles[1], tiles[0])
    for k, value in enumerate((even, odd)):
        y = dot3((wyi[k, 0], wyi[k, 1]), split(value.reshape(2 * n, 2 * n)))
        rows = jnp.concatenate(
            [
                jnp.concatenate([y[:n, a * n : (a + 1) * n], y[n:, a * n : (a + 1) * n]], axis=1)
                for a in range(2)
            ],
            axis=0,
        )
        x = dot3(split(rows), (wzi[0], wzi[1]))
        for r in range(2):
            part = x[:, r * n : (r + 1) * n].reshape(2, n, n)
            out[2 * step + k, r] = part + fxc[...] * (own[2 * step + k, r] + arrived[2 * step + k, r])


def place_kernel(pieces, slot, *rest):
    parts, out, done = rest[: len(pieces)], rest[-2], rest[-1]
    half = out.shape[0] // 2
    pool = lax.axis_index("pool")
    copies = []
    for (start, other), part in zip(pieces, parts):
        first = half * (1 - pool if other else pool) + start
        for k in range(part.shape[0]):
            copies.append(pltpu.make_async_copy(part.at[k], out.at[slot[first + k]], done.at[len(copies)]))
    for copy in copies:
        copy.start()
    for copy in copies:
        copy.wait()


def frequency(index, length):
    return ((index + length // 2) % length - length // 2).astype(F32)


def column_kernel(cutoff_mask, length):
    width = cutoff_mask.shape[1]
    start = lax.axis_index("slab") * width
    full_index = jnp.arange(length, dtype=jnp.int32)
    dealt_index = full_index.reshape(-1, 2).T.reshape(-1)
    part_index = start + jnp.arange(width, dtype=jnp.int32)
    first_square = frequency(dealt_index, length) ** 2
    part_square = frequency(part_index, length) ** 2
    last_square = frequency(full_index, length) ** 2
    total = part_square[:, None, None] + first_square[None, :, None] + last_square[None, None, :]
    unit = (2.0 * math.pi / length) ** 2
    mask = cutoff_mask.reshape(-1, 2, width, length).transpose(2, 1, 0, 3).reshape(width, length, length).astype(F32)
    scale = 1.0 / float(length) ** 3
    return (4.0 * math.pi * mask / (unit * total + 0.25)) * scale


RESIDENT = pl.BlockSpec(memory_space=pltpu.VMEM)


def taking(us):
    return pl.CostEstimate(flops=int(us * 1e8), bytes_accessed=0, transcendentals=0)


def per_device(drho_part, fxc, cutoff_mask, owner_table):
    local = drho_part[0]
    slots, _, planes, n, _ = local.shape
    devices = lax.axis_size("slab")
    mine = slots // 2
    tile = (2, planes, n, n)
    swap = [(0, 1), (1, 0)]
    limit = lambda share: pltpu.CompilerParams(vmem_limit_bytes=share << 20)
    ahead = [(0, mine // 2), (mine // 2, mine // 2)]
    behind = ahead

    forward = dft(n, -1.0)
    inverse = dft(n, 1.0)
    dealt = [dealt_rows(n, devices, s) for s in (False, True)]
    wz = jnp.asarray(halves(forward.T))
    wzi = jnp.asarray(halves(inverse.T))
    wy = jnp.asarray(np.stack([halves(forward[rows]) for rows in dealt]))
    wyi = jnp.asarray(np.stack([halves(inverse[:, rows]) for rows in dealt]))
    wx = jnp.asarray(np.stack([halves(w) for w in dft_halves(n, -1.0)]))
    wxi = jnp.asarray(np.stack([halves(w.T) for w in dft_halves(n, -1.0)]))

    far = pl.BlockSpec(memory_space=pl.ANY)
    scalars = pl.BlockSpec(memory_space=pltpu.SMEM)
    parts = lambda count: jax.ShapeDtypeStruct((count, *tile), F32)

    def collected(other, share):
        return pl.pallas_call(
            functools.partial(collect_kernel, ahead, other),
            out_shape=tuple(parts(count) for _, count in ahead),
            in_specs=[far],
            out_specs=(RESIDENT,) * len(ahead),
            scratch_shapes=[pltpu.SemaphoreType.DMA((len(ahead),))],
            compiler_params=limit(share),
            cost_estimate=taking(1),
        )(local)

    arrived = []
    for sent in collected(True, 49):
        arrived.append(lax.ppermute(sent, "pool", swap))
    own = collected(False, 49)

    shape = (devices // 2, 2, planes, mine // 2, 8, n)
    spectrum = None
    for c, (start, count) in enumerate(ahead):
        operands = [own[c], arrived[c], wz, wy]
        specs = [RESIDENT] * 4
        aliases = {}
        if spectrum is not None:
            aliases = {len(operands): 0}
            operands.append(spectrum)
            specs.append(far)
        spectrum = pl.pallas_call(
            forward_kernel,
            out_shape=jax.ShapeDtypeStruct(shape, F32),
            grid=(count // 2,),
            in_specs=specs,
            out_specs=pl.BlockSpec(
                (devices // 2, 2, planes, 1, 8, n), lambda i, start=start: (0, 0, 0, start // 2 + i, 0, 0)
            ),
            input_output_aliases=aliases,
            compiler_params=limit(40),
            cost_estimate=taking(0.6 * count),
        )(*operands)

    kernel = column_kernel(cutoff_mask, n)
    index = jnp.arange(slots, dtype=jnp.int32)
    slot = jnp.sum(jnp.where(owner_table[None, :] == index[:, None], index[None, :], 0), axis=1)
    flat = (devices, planes * (mine // 2) * 8, n)
    columns = lax.all_to_all(spectrum.reshape(flat), "slab", split_axis=0, concat_axis=0, tiled=True)
    columns = columns.reshape(n, mine // 2, 8, n)
    columns = pl.pallas_call(
        middle_kernel,
        out_shape=jax.ShapeDtypeStruct(columns.shape, F32),
        grid=(mine // 2,),
        in_specs=[RESIDENT] * 4,
        out_specs=RESIDENT,
        scratch_shapes=[pltpu.VMEM((n * 8, n), F32), pltpu.VMEM((n * 8, n), F32)],
        compiler_params=limit(40),
        cost_estimate=taking(4),
        name="middle",
    )(columns, wx, wxi, kernel)
    columns = lax.all_to_all(columns.reshape(flat), "slab", split_axis=0, concat_axis=0, tiled=True)
    columns = columns.reshape(shape)

    results, others = [], []
    for start, count in behind:
        k = ahead.index((start, count))
        results.append(
            pl.pallas_call(
                functools.partial(backward_kernel, start),
                out_shape=parts(count),
                grid=(count // 2,),
                in_specs=[RESIDENT] * 6,
                out_specs=RESIDENT,
                compiler_params=limit(40),
                cost_estimate=taking(0.6 * count),
            )(columns, wyi, wzi, fxc, own[k], arrived[k])
        )
        others.append(lax.ppermute(results[-1], "pool", swap))

    def placed(pieces, arrays, out=None):
        aliases = {} if out is None else {1 + len(arrays): 0}
        kept = [] if out is None else [out]
        return pl.pallas_call(
            functools.partial(place_kernel, pieces),
            out_shape=jax.ShapeDtypeStruct(local.shape, F32),
            in_specs=[scalars] + [RESIDENT] * len(arrays) + [far] * len(kept),
            out_specs=far,
            scratch_shapes=[pltpu.SemaphoreType.DMA((sum(a.shape[0] for a in arrays),))],
            input_output_aliases=aliases,
            compiler_params=limit(40),
            cost_estimate=taking(1),
        )(slot, *arrays, *kept)

    starts = [start for start, _ in behind]
    out = placed([(starts[0], False), (starts[1], False), (starts[0], True)], [*results, others[0]])
    return placed([(starts[1], True)], [others[1]], out)


def solution(mesh):
    placed = (
        P("pool", "group", None, "slab", None, None),
        P("slab", None, None),
        P(None, "slab", None),
        P("group"),
    )

    return jax.shard_map(
        per_device,
        mesh=mesh,
        in_specs=placed,
        out_specs=P("group", None, "slab", None, None),
        check_vma=False,
    )
```

```python
import functools
import math

import jax
import jax.numpy as jnp
import numpy as np
from jax import lax
from jax.experimental import pallas as pl
from jax.experimental.pallas import tpu as pltpu
from jax.sharding import PartitionSpec as P


F32 = jnp.float32
BF16 = jnp.bfloat16


def halves(table):
    high = table.astype(BF16)
    low = (table - high.astype(np.float64)).astype(BF16)
    return np.stack([high, low])


def dft(length, sign):
    index = np.arange(length)
    angle = 2.0 * np.pi * ((index[:, None] * index[None, :]) % length) / length
    cosine, sine = np.cos(angle), sign * np.sin(angle)
    return np.block([[cosine, -sine], [sine, cosine]])


def dft_halves(length, sign):
    outputs = np.arange(length).reshape(-1, 2).T
    parts = []
    for k in outputs:
        angle = 2.0 * np.pi * ((k[:, None] * np.arange(length // 2)[None, :]) % length) / length
        cosine, sine = np.cos(angle), sign * np.sin(angle)
        parts.append(np.block([[cosine, -sine], [sine, cosine]]))
    return parts


def dealt_rows(length, devices, swap):
    width = length // devices
    rows = []
    for s in range(devices):
        s = s ^ 1 if swap else s
        rows += [r * length + s * width + b for r in range(2) for b in range(width)]
    return np.array(rows)


def table_first(table, value):
    dot = functools.partial(jnp.dot, preferred_element_type=F32)
    high, low = split(value)
    m = table.shape[1]
    both = dot(jnp.concatenate([table[0], table[1]], axis=0), high)
    return both[:m] + (both[m:] + dot(table[0], low))


def table_last(value, table):
    dot = functools.partial(jnp.dot, preferred_element_type=F32)
    high, low = split(value)
    m = value.shape[0]
    both = dot(jnp.concatenate([high, low], axis=0), table[0])
    return both[:m] + (both[m:] + dot(high, table[1]))


def split(value):
    high = value.astype(BF16)
    return high, (value - high.astype(F32)).astype(BF16)


def collect_kernel(parts, other, local, *rest):
    kept, done = rest[-1 - len(parts) : -1], rest[-1]
    pool = lax.axis_index("pool")
    first = local.shape[0] // 2 * (1 - pool if other else pool)
    copies = [
        pltpu.make_async_copy(local.at[pl.ds(first + start, count)], part, done.at[k])
        for k, ((start, count), part) in enumerate(zip(parts, kept))
    ]
    for copy in copies:
        copy.start()
    for copy in copies:
        copy.wait()


def transformed(x, wz, wy):
    n = x.shape[-1]
    rows = jnp.concatenate([x[:, 0].reshape(4 * n, n), x[:, 1].reshape(4 * n, n)], axis=1)
    y = table_last(rows, wz)
    mixed = []
    for k in range(2):
        first, second = y[2 * k * n : (2 * k + 1) * n], y[(2 * k + 1) * n : (2 * k + 2) * n]
        real = jnp.concatenate([first[:, :n], second[:, :n]], axis=1)
        imag = jnp.concatenate([first[:, n:], second[:, n:]], axis=1)
        mixed.append(table_first(wy[k], jnp.concatenate([real, imag], axis=0)).reshape(-1, 8, 2 * n))
    even, odd = mixed
    lower = lax.broadcasted_iota(jnp.int32, even.shape, 1) < 4
    return jnp.where(lower, even, odd), jnp.where(lower, odd, even)


def forward_first_kernel(own, arrived, wz, wy, tiles):
    n = own.shape[-1]
    step = pl.program_id(0)
    pair = pl.ds(2 * step, 2)
    for j, value in enumerate(transformed(own[pair] + arrived[pair], wz[...], wy[...])):
        for a in range(2):
            tiles[:, j, a, step] = value[:, :, a * n : (a + 1) * n]


def forward_second_kernel(own, arrived, wz, wy, tiles, spectrum, later, done):
    n = own.shape[-1]
    step = pl.program_id(0)
    last = pl.num_programs(0) - 1
    ready = tiles.shape[3]
    earlier = pltpu.make_async_copy(tiles, spectrum.at[:, :, :, pl.ds(0, ready)], done.at[0])

    @pl.when(step == 0)
    def _():
        earlier.start()

    pair = pl.ds(2 * step, 2)
    for j, value in enumerate(transformed(own[pair] + arrived[pair], wz[...], wy[...])):
        for a in range(2):
            later[step, :, j, a] = value[:, :, a * n : (a + 1) * n]

    sent = [
        pltpu.make_async_copy(later.at[i], spectrum.at[:, :, :, ready + i], done.at[1 + i])
        for i in range(spectrum.shape[3] - ready)
    ]
    for i, copy in enumerate(sent):

        @pl.when(step == i)
        def _(copy=copy):
            copy.start()

    @pl.when(step == last)
    def _():
        earlier.wait()
        for copy in sent:
            copy.wait()


def by_parts(table, even, odd):
    dot = functools.partial(jnp.dot, preferred_element_type=F32)
    (even_high, even_low), (odd_high, odd_low) = split(even), split(odd)
    main = [
        dot(jnp.concatenate([table[i, 0], table[i, 0]], axis=1), jnp.concatenate([high, low], axis=0))
        for i, (high, low) in enumerate(((even_high, even_low), (odd_high, odd_low)))
    ]
    zero = jnp.zeros(table.shape[2:], BF16)
    low = jnp.concatenate(
        [jnp.concatenate([table[0, 1], zero], axis=1), jnp.concatenate([zero, table[1, 1]], axis=1)], axis=0
    )
    return jnp.concatenate(main, axis=0) + dot(low, jnp.concatenate([even_high, odd_high], axis=0))


def middle_kernel(columns, wx, wxi, kernel, out, rows, back):
    n = kernel.shape[-1]
    length = kernel.shape[1]
    half = length // 2
    step = pl.program_id(0)
    rows[...] = columns[:, step].reshape(rows.shape)
    grab = lambda j: rows[pl.ds(j, length, stride=8), :]
    order = [(p, b) for p in range(2) for b in range(2)]
    fields = [jnp.concatenate([grab(4 * p + 2 * r + b) for p, b in order], axis=1) for r in range(2)]
    total = jnp.concatenate([f[:half] + f[half:] for f in fields], axis=0)
    difference = jnp.concatenate([f[:half] - f[half:] for f in fields], axis=0)
    spectrum = by_parts(wx, total, difference)
    both = jnp.concatenate([kernel[0], kernel[1]] * 2, axis=1)
    both = jnp.concatenate([both[:half], both[:half], both[half:], both[half:]], axis=0)
    spectrum = spectrum * both
    result = by_parts(wxi, spectrum[:length], spectrum[length:])
    even, odd = result[:length], result[length:]
    sides = (even + odd, even - odd)
    for i, (p, b) in enumerate(order):
        for r in range(2):
            for h, side in enumerate(sides):
                back[pl.ds(h * half * 8 + 4 * p + 2 * r + b, half, stride=8), :] = side[
                    r * half : (r + 1) * half, i * n : (i + 1) * n
                ]
    out[:, step] = back[...].reshape(length, 8, n)


def backward_kernel(start, columns, wyi, wzi, fxc, own, arrived, out):
    n = fxc.shape[-1]
    step = pl.program_id(0)
    place = start // 2 + step
    tiles = [jnp.concatenate([columns[:, j, a, place] for a in range(2)], axis=-1) for j in range(2)]
    lower = lax.broadcasted_iota(jnp.int32, tiles[0].shape, 1) < 4
    even = jnp.where(lower, tiles[0], tiles[1])
    odd = jnp.where(lower, tiles[1], tiles[0])
    rows = []
    for k, value in enumerate((even, odd)):
        y = table_first(wyi[k], value.reshape(2 * n, 2 * n))
        for a in range(2):
            rows.append(jnp.concatenate([y[:n, a * n : (a + 1) * n], y[n:, a * n : (a + 1) * n]], axis=1))
    x = table_last(jnp.concatenate(rows, axis=0), wzi[...])
    for k in range(2):
        for r in range(2):
            part = x[2 * k * n : (2 * k + 2) * n, r * n : (r + 1) * n].reshape(2, n, n)
            out[2 * step + k, r] = part + fxc[...] * (own[2 * step + k, r] + arrived[2 * step + k, r])


def place_kernel(pieces, slot, *rest):
    parts, out, done = rest[: len(pieces)], rest[-2], rest[-1]
    half = out.shape[0] // 2
    pool = lax.axis_index("pool")
    copies = []
    for (start, other), part in zip(pieces, parts):
        first = half * (1 - pool if other else pool) + start
        for k in range(part.shape[0]):
            copies.append(pltpu.make_async_copy(part.at[k], out.at[slot[first + k]], done.at[len(copies)]))
    for copy in copies:
        copy.start()
    for copy in copies:
        copy.wait()


def frequency(index, length):
    return ((index + length // 2) % length - length // 2).astype(F32)


def column_kernel(cutoff_mask, length):
    width = cutoff_mask.shape[1]
    start = lax.axis_index("slab") * width
    full_index = jnp.arange(length, dtype=jnp.int32)
    dealt_index = full_index.reshape(-1, 2).T.reshape(-1)
    part_index = start + jnp.arange(width, dtype=jnp.int32)
    first_square = frequency(dealt_index, length) ** 2
    part_square = frequency(part_index, length) ** 2
    last_square = frequency(full_index, length) ** 2
    total = part_square[:, None, None] + first_square[None, :, None] + last_square[None, None, :]
    unit = (2.0 * math.pi / length) ** 2
    mask = cutoff_mask.reshape(-1, 2, width, length).transpose(2, 1, 0, 3).reshape(width, length, length).astype(F32)
    scale = 1.0 / float(length) ** 3
    return (4.0 * math.pi * mask / (unit * total + 0.25)) * scale


RESIDENT = pl.BlockSpec(memory_space=pltpu.VMEM)


def taking(us):
    return pl.CostEstimate(flops=int(us * 1e8), bytes_accessed=0, transcendentals=0)


def per_device(drho_part, fxc, cutoff_mask, owner_table):
    local = drho_part[0]
    slots, _, planes, n, _ = local.shape
    devices = lax.axis_size("slab")
    mine = slots // 2
    tile = (2, planes, n, n)
    swap = [(0, 1), (1, 0)]
    limit = lambda share: pltpu.CompilerParams(vmem_limit_bytes=share << 20)
    ahead = [(0, mine // 2), (mine // 2, mine // 2)]
    behind = ahead

    forward = dft(n, -1.0)
    inverse = dft(n, 1.0)
    dealt = [dealt_rows(n, devices, s) for s in (False, True)]
    wz = jnp.asarray(halves(forward.T))
    wzi = jnp.asarray(halves(inverse.T))
    wy = jnp.asarray(np.stack([halves(forward[rows]) for rows in dealt]))
    wyi = jnp.asarray(np.stack([halves(inverse[:, rows]) for rows in dealt]))
    wx = jnp.asarray(np.stack([halves(w) for w in dft_halves(n, -1.0)]))
    wxi = jnp.asarray(np.stack([halves(w.T) for w in dft_halves(n, -1.0)]))

    far = pl.BlockSpec(memory_space=pl.ANY)
    scalars = pl.BlockSpec(memory_space=pltpu.SMEM)
    parts = lambda count: jax.ShapeDtypeStruct((count, *tile), F32)

    def collected(other, share):
        return pl.pallas_call(
            functools.partial(collect_kernel, ahead, other),
            out_shape=tuple(parts(count) for _, count in ahead),
            in_specs=[far],
            out_specs=(RESIDENT,) * len(ahead),
            scratch_shapes=[pltpu.SemaphoreType.DMA((len(ahead),))],
            compiler_params=limit(share),
            cost_estimate=taking(1),
        )(local)

    arrived = []
    for sent in collected(True, 49):
        arrived.append(lax.ppermute(sent, "pool", swap))
    own = collected(False, 49)

    shape = (devices // 2, 2, planes, mine // 2, 8, n)
    ready = ahead[0][1] // 2
    tiles = pl.pallas_call(
        forward_first_kernel,
        out_shape=jax.ShapeDtypeStruct((*shape[:3], ready, *shape[4:]), F32),
        grid=(ready,),
        in_specs=[RESIDENT] * 4,
        out_specs=RESIDENT,
        compiler_params=limit(40),
        cost_estimate=taking(2.4),
        name="forward0",
    )(own[0], arrived[0], wz, wy)
    later = shape[3] - ready
    spectrum = pl.pallas_call(
        forward_second_kernel,
        out_shape=jax.ShapeDtypeStruct(shape, F32),
        grid=(later,),
        in_specs=[RESIDENT] * 5,
        out_specs=far,
        scratch_shapes=[
            pltpu.VMEM((later, *shape[:3], *shape[4:]), F32),
            pltpu.SemaphoreType.DMA((1 + later,)),
        ],
        compiler_params=limit(40),
        cost_estimate=taking(2.4),
        name="forward1",
    )(own[1], arrived[1], wz, wy, tiles)

    kernel = column_kernel(cutoff_mask, n)
    index = jnp.arange(slots, dtype=jnp.int32)
    slot = jnp.sum(jnp.where(owner_table[None, :] == index[:, None], index[None, :], 0), axis=1)
    flat = (devices, planes * (mine // 2) * 8, n)
    columns = lax.all_to_all(spectrum.reshape(flat), "slab", split_axis=0, concat_axis=0, tiled=True)
    columns = columns.reshape(n, mine // 2, 8, n)
    columns = pl.pallas_call(
        middle_kernel,
        out_shape=jax.ShapeDtypeStruct(columns.shape, F32),
        grid=(mine // 2,),
        in_specs=[RESIDENT] * 4,
        out_specs=RESIDENT,
        scratch_shapes=[pltpu.VMEM((n * 8, n), F32), pltpu.VMEM((n * 8, n), F32)],
        compiler_params=limit(40),
        cost_estimate=taking(4),
        name="middle",
    )(columns, wx, wxi, kernel)
    columns = lax.all_to_all(columns.reshape(flat), "slab", split_axis=0, concat_axis=0, tiled=True)
    columns = columns.reshape(shape)

    results, others = [], []
    for start, count in behind:
        k = ahead.index((start, count))
        results.append(
            pl.pallas_call(
                functools.partial(backward_kernel, start),
                out_shape=parts(count),
                grid=(count // 2,),
                in_specs=[RESIDENT] * 6,
                out_specs=RESIDENT,
                compiler_params=limit(40),
                cost_estimate=taking(0.6 * count),
            )(columns, wyi, wzi, fxc, own[k], arrived[k])
        )
        others.append(lax.ppermute(results[-1], "pool", swap))

    def placed(pieces, arrays, out=None):
        aliases = {} if out is None else {1 + len(arrays): 0}
        kept = [] if out is None else [out]
        return pl.pallas_call(
            functools.partial(place_kernel, pieces),
            out_shape=jax.ShapeDtypeStruct(local.shape, F32),
            in_specs=[scalars] + [RESIDENT] * len(arrays) + [far] * len(kept),
            out_specs=far,
            scratch_shapes=[pltpu.SemaphoreType.DMA((sum(a.shape[0] for a in arrays),))],
            input_output_aliases=aliases,
            compiler_params=limit(40),
            cost_estimate=taking(1),
        )(slot, *arrays, *kept)

    starts = [start for start, _ in behind]
    out = placed([(starts[0], False), (starts[1], False), (starts[0], True)], [*results, others[0]])
    return placed([(starts[1], True)], [others[1]], out)


def solution(mesh):
    placed = (
        P("pool", "group", None, "slab", None, None),
        P("slab", None, None),
        P(None, "slab", None),
        P("group"),
    )

    return jax.shard_map(
        per_device,
        mesh=mesh,
        in_specs=placed,
        out_specs=P("group", None, "slab", None, None),
        check_vma=False,
    )
```

```python
import functools
import math

import jax
import jax.numpy as jnp
import numpy as np
from jax import lax
from jax.experimental import pallas as pl
from jax.experimental.pallas import tpu as pltpu
from jax.sharding import PartitionSpec as P


F32 = jnp.float32
BF16 = jnp.bfloat16


def halves(table):
    high = table.astype(BF16)
    low = (table - high.astype(np.float64)).astype(BF16)
    return np.stack([high, low])


def dft(length, sign):
    index = np.arange(length)
    angle = 2.0 * np.pi * ((index[:, None] * index[None, :]) % length) / length
    cosine, sine = np.cos(angle), sign * np.sin(angle)
    return np.block([[cosine, -sine], [sine, cosine]])


def dft_halves(length, sign):
    outputs = np.arange(length).reshape(-1, 2).T
    parts = []
    for k in outputs:
        angle = 2.0 * np.pi * ((k[:, None] * np.arange(length // 2)[None, :]) % length) / length
        cosine, sine = np.cos(angle), sign * np.sin(angle)
        parts.append(np.block([[cosine, -sine], [sine, cosine]]))
    return parts


def dealt_rows(length, devices, swap):
    width = length // devices
    rows = []
    for s in range(devices):
        s = s ^ 1 if swap else s
        rows += [r * length + s * width + b for r in range(2) for b in range(width)]
    return np.array(rows)


def table_first(table, value):
    dot = functools.partial(jnp.dot, preferred_element_type=F32)
    high, low = split(value)
    m = table.shape[1]
    both = dot(jnp.concatenate([table[0], table[1]], axis=0), high)
    return both[:m] + (both[m:] + dot(table[0], low))


def table_last(value, table):
    dot = functools.partial(jnp.dot, preferred_element_type=F32)
    high, low = split(value)
    m = value.shape[0]
    both = dot(jnp.concatenate([high, low], axis=0), table[0])
    return both[:m] + (both[m:] + dot(high, table[1]))


def split(value):
    high = value.astype(BF16)
    return high, (value - high.astype(F32)).astype(BF16)


def collect_kernel(pieces, local, *rest):
    kept, done = rest[-1 - len(pieces) : -1], rest[-1]
    half = local.shape[0] // 2
    pool = lax.axis_index("pool")
    copies = [
        pltpu.make_async_copy(
            local.at[pl.ds(half * (1 - pool if other else pool) + start, count)], part, done.at[k]
        )
        for k, ((start, count, other), part) in enumerate(zip(pieces, kept))
    ]
    for copy in copies:
        copy.start()
    for copy in copies:
        copy.wait()


def transformed(x, wz, wy):
    n = x.shape[-1]
    rows = jnp.concatenate([x[:, 0].reshape(4 * n, n), x[:, 1].reshape(4 * n, n)], axis=1)
    y = table_last(rows, wz)
    mixed = []
    for k in range(2):
        first, second = y[2 * k * n : (2 * k + 1) * n], y[(2 * k + 1) * n : (2 * k + 2) * n]
        real = jnp.concatenate([first[:, :n], second[:, :n]], axis=1)
        imag = jnp.concatenate([first[:, n:], second[:, n:]], axis=1)
        mixed.append(table_first(wy[k], jnp.concatenate([real, imag], axis=0)).reshape(-1, 8, 2 * n))
    even, odd = mixed
    lower = lax.broadcasted_iota(jnp.int32, even.shape, 1) < 4
    return jnp.where(lower, even, odd), jnp.where(lower, odd, even)


def forward_first_kernel(own, arrived, wz, wy, tiles):
    n = own.shape[-1]
    step = pl.program_id(0)
    pair = pl.ds(2 * step, 2)
    for j, value in enumerate(transformed(own[pair] + arrived[pair], wz[...], wy[...])):
        for a in range(2):
            tiles[:, j, a, step] = value[:, :, a * n : (a + 1) * n]


def forward_second_kernel(own, arrived, wz, wy, tiles, spectrum, later, done):
    n = own.shape[-1]
    step = pl.program_id(0)
    last = pl.num_programs(0) - 1
    ready = tiles.shape[3]
    earlier = pltpu.make_async_copy(tiles, spectrum.at[:, :, :, pl.ds(0, ready)], done.at[0])

    @pl.when(step == 0)
    def _():
        earlier.start()

    pair = pl.ds(2 * step, 2)
    for j, value in enumerate(transformed(own[pair] + arrived[pair], wz[...], wy[...])):
        for a in range(2):
            later[step, :, j, a] = value[:, :, a * n : (a + 1) * n]

    sent = [
        pltpu.make_async_copy(later.at[i], spectrum.at[:, :, :, ready + i], done.at[1 + i])
        for i in range(spectrum.shape[3] - ready)
    ]
    for i, copy in enumerate(sent):

        @pl.when(step == i)
        def _(copy=copy):
            copy.start()

    @pl.when(step == last)
    def _():
        earlier.wait()
        for copy in sent:
            copy.wait()


def by_parts(table, even, odd):
    dot = functools.partial(jnp.dot, preferred_element_type=F32)
    (even_high, even_low), (odd_high, odd_low) = split(even), split(odd)
    main = [
        dot(jnp.concatenate([table[i, 0], table[i, 0]], axis=1), jnp.concatenate([high, low], axis=0))
        for i, (high, low) in enumerate(((even_high, even_low), (odd_high, odd_low)))
    ]
    zero = jnp.zeros(table.shape[2:], BF16)
    low = jnp.concatenate(
        [jnp.concatenate([table[0, 1], zero], axis=1), jnp.concatenate([zero, table[1, 1]], axis=1)], axis=0
    )
    return jnp.concatenate(main, axis=0) + dot(low, jnp.concatenate([even_high, odd_high], axis=0))


def middle_kernel(columns, wx, wxi, kernel, out, rows, back):
    n = kernel.shape[-1]
    length = kernel.shape[1]
    half = length // 2
    step = pl.program_id(0)
    rows[...] = columns[:, step].reshape(rows.shape)
    grab = lambda j: rows[pl.ds(j, length, stride=8), :]
    order = [(p, b) for p in range(2) for b in range(2)]
    fields = [jnp.concatenate([grab(4 * p + 2 * r + b) for p, b in order], axis=1) for r in range(2)]
    total = jnp.concatenate([f[:half] + f[half:] for f in fields], axis=0)
    difference = jnp.concatenate([f[:half] - f[half:] for f in fields], axis=0)
    spectrum = by_parts(wx, total, difference)
    both = jnp.concatenate([kernel[0], kernel[1]] * 2, axis=1)
    both = jnp.concatenate([both[:half], both[:half], both[half:], both[half:]], axis=0)
    spectrum = spectrum * both
    result = by_parts(wxi, spectrum[:length], spectrum[length:])
    even, odd = result[:length], result[length:]
    sides = (even + odd, even - odd)
    for i, (p, b) in enumerate(order):
        for r in range(2):
            for h, side in enumerate(sides):
                back[pl.ds(h * half * 8 + 4 * p + 2 * r + b, half, stride=8), :] = side[
                    r * half : (r + 1) * half, i * n : (i + 1) * n
                ]
    out[:, step] = back[...].reshape(length, 8, n)


def backward_kernel(start, columns, wyi, wzi, fxc, own, arrived, out):
    n = fxc.shape[-1]
    step = pl.program_id(0)
    place = start // 2 + step
    tiles = [jnp.concatenate([columns[:, j, a, place] for a in range(2)], axis=-1) for j in range(2)]
    lower = lax.broadcasted_iota(jnp.int32, tiles[0].shape, 1) < 4
    even = jnp.where(lower, tiles[0], tiles[1])
    odd = jnp.where(lower, tiles[1], tiles[0])
    rows = []
    for k, value in enumerate((even, odd)):
        y = table_first(wyi[k], value.reshape(2 * n, 2 * n))
        for a in range(2):
            rows.append(jnp.concatenate([y[:n, a * n : (a + 1) * n], y[n:, a * n : (a + 1) * n]], axis=1))
    x = table_last(jnp.concatenate(rows, axis=0), wzi[...])
    for k in range(2):
        for r in range(2):
            part = x[2 * k * n : (2 * k + 2) * n, r * n : (r + 1) * n].reshape(2, n, n)
            out[2 * step + k, r] = part + fxc[...] * (own[2 * step + k, r] + arrived[2 * step + k, r])


def place_kernel(pieces, slot, *rest):
    parts, out, done = rest[: len(pieces)], rest[-2], rest[-1]
    half = out.shape[0] // 2
    pool = lax.axis_index("pool")
    copies = []
    for (start, other), part in zip(pieces, parts):
        first = half * (1 - pool if other else pool) + start
        for k in range(part.shape[0]):
            copies.append(pltpu.make_async_copy(part.at[k], out.at[slot[first + k]], done.at[len(copies)]))
    for copy in copies:
        copy.start()
    for copy in copies:
        copy.wait()


def frequency(index, length):
    return ((index + length // 2) % length - length // 2).astype(F32)


def column_kernel(cutoff_mask, length):
    width = cutoff_mask.shape[1]
    start = lax.axis_index("slab") * width
    full_index = jnp.arange(length, dtype=jnp.int32)
    dealt_index = full_index.reshape(-1, 2).T.reshape(-1)
    part_index = start + jnp.arange(width, dtype=jnp.int32)
    first_square = frequency(dealt_index, length) ** 2
    part_square = frequency(part_index, length) ** 2
    last_square = frequency(full_index, length) ** 2
    total = part_square[:, None, None] + first_square[None, :, None] + last_square[None, None, :]
    unit = (2.0 * math.pi / length) ** 2
    mask = cutoff_mask.reshape(-1, 2, width, length).transpose(2, 1, 0, 3).reshape(width, length, length).astype(F32)
    scale = 1.0 / float(length) ** 3
    return (4.0 * math.pi * mask / (unit * total + 0.25)) * scale


RESIDENT = pl.BlockSpec(memory_space=pltpu.VMEM)


def taking(us):
    return pl.CostEstimate(flops=int(us * 1e8), bytes_accessed=0, transcendentals=0)


def per_device(drho_part, fxc, cutoff_mask, owner_table):
    local = drho_part[0]
    slots, _, planes, n, _ = local.shape
    devices = lax.axis_size("slab")
    mine = slots // 2
    tile = (2, planes, n, n)
    swap = [(0, 1), (1, 0)]
    limit = lambda share: pltpu.CompilerParams(vmem_limit_bytes=share << 20)
    ahead = [(0, mine // 2), (mine // 2, mine // 2)]
    behind = ahead

    forward = dft(n, -1.0)
    inverse = dft(n, 1.0)
    dealt = [dealt_rows(n, devices, s) for s in (False, True)]
    wz = jnp.asarray(halves(forward.T))
    wzi = jnp.asarray(halves(inverse.T))
    wy = jnp.asarray(np.stack([halves(forward[rows]) for rows in dealt]))
    wyi = jnp.asarray(np.stack([halves(inverse[:, rows]) for rows in dealt]))
    wx = jnp.asarray(np.stack([halves(w) for w in dft_halves(n, -1.0)]))
    wxi = jnp.asarray(np.stack([halves(w.T) for w in dft_halves(n, -1.0)]))

    far = pl.BlockSpec(memory_space=pl.ANY)
    scalars = pl.BlockSpec(memory_space=pltpu.SMEM)
    parts = lambda count: jax.ShapeDtypeStruct((count, *tile), F32)

    def collected(pieces, *earlier):
        return pl.pallas_call(
            functools.partial(collect_kernel, pieces),
            out_shape=tuple(parts(count) for _, count, _ in pieces),
            in_specs=[far] * (1 + len(earlier)),
            out_specs=(RESIDENT,) * len(pieces),
            scratch_shapes=[pltpu.SemaphoreType.DMA((len(pieces),))],
            compiler_params=limit(49),
            cost_estimate=taking(1),
        )(local, *earlier)

    (first,) = collected([(*ahead[0], True)])
    second, *own = collected([(*ahead[1], True), (*ahead[0], False), (*ahead[1], False)], first)
    arrived = []
    for sent in (first, second):
        arrived.append(lax.ppermute(sent, "pool", swap))

    shape = (devices // 2, 2, planes, mine // 2, 8, n)
    ready = ahead[0][1] // 2
    tiles = pl.pallas_call(
        forward_first_kernel,
        out_shape=jax.ShapeDtypeStruct((*shape[:3], ready, *shape[4:]), F32),
        grid=(ready,),
        in_specs=[RESIDENT] * 4,
        out_specs=RESIDENT,
        compiler_params=limit(40),
        cost_estimate=taking(2.4),
        name="forward0",
    )(own[0], arrived[0], wz, wy)
    later = shape[3] - ready
    spectrum = pl.pallas_call(
        forward_second_kernel,
        out_shape=jax.ShapeDtypeStruct(shape, F32),
        grid=(later,),
        in_specs=[RESIDENT] * 5,
        out_specs=far,
        scratch_shapes=[
            pltpu.VMEM((later, *shape[:3], *shape[4:]), F32),
            pltpu.SemaphoreType.DMA((1 + later,)),
        ],
        compiler_params=limit(40),
        cost_estimate=taking(2.4),
        name="forward1",
    )(own[1], arrived[1], wz, wy, tiles)

    kernel = column_kernel(cutoff_mask, n)
    index = jnp.arange(slots, dtype=jnp.int32)
    slot = jnp.sum(jnp.where(owner_table[None, :] == index[:, None], index[None, :], 0), axis=1)
    flat = (devices, planes * (mine // 2) * 8, n)
    columns = lax.all_to_all(spectrum.reshape(flat), "slab", split_axis=0, concat_axis=0, tiled=True)
    columns = columns.reshape(n, mine // 2, 8, n)
    columns = pl.pallas_call(
        middle_kernel,
        out_shape=jax.ShapeDtypeStruct(columns.shape, F32),
        grid=(mine // 2,),
        in_specs=[RESIDENT] * 4,
        out_specs=RESIDENT,
        scratch_shapes=[pltpu.VMEM((n * 8, n), F32), pltpu.VMEM((n * 8, n), F32)],
        compiler_params=limit(40),
        cost_estimate=taking(4),
        name="middle",
    )(columns, wx, wxi, kernel)
    columns = lax.all_to_all(columns.reshape(flat), "slab", split_axis=0, concat_axis=0, tiled=True)
    columns = columns.reshape(shape)

    results, others = [], []
    for start, count in behind:
        k = ahead.index((start, count))
        results.append(
            pl.pallas_call(
                functools.partial(backward_kernel, start),
                out_shape=parts(count),
                grid=(count // 2,),
                in_specs=[RESIDENT] * 6,
                out_specs=RESIDENT,
                compiler_params=limit(40),
                cost_estimate=taking(0.6 * count),
            )(columns, wyi, wzi, fxc, own[k], arrived[k])
        )
        others.append(lax.ppermute(results[-1], "pool", swap))

    def placed(pieces, arrays, out=None):
        aliases = {} if out is None else {1 + len(arrays): 0}
        kept = [] if out is None else [out]
        return pl.pallas_call(
            functools.partial(place_kernel, pieces),
            out_shape=jax.ShapeDtypeStruct(local.shape, F32),
            in_specs=[scalars] + [RESIDENT] * len(arrays) + [far] * len(kept),
            out_specs=far,
            scratch_shapes=[pltpu.SemaphoreType.DMA((sum(a.shape[0] for a in arrays),))],
            input_output_aliases=aliases,
            compiler_params=limit(40),
            cost_estimate=taking(1),
        )(slot, *arrays, *kept)

    starts = [start for start, _ in behind]
    out = placed([(start, False) for start in starts], results)
    return placed([(start, True) for start in starts], others, out)


def solution(mesh):
    placed = (
        P("pool", "group", None, "slab", None, None),
        P("slab", None, None),
        P(None, "slab", None),
        P("group"),
    )

    return jax.shard_map(
        per_device,
        mesh=mesh,
        in_specs=placed,
        out_specs=P("group", None, "slab", None, None),
        check_vma=False,
    )
```

```python
import functools
import math

import jax
import jax.numpy as jnp
import numpy as np
from jax import lax
from jax.experimental import pallas as pl
from jax.experimental.pallas import tpu as pltpu
from jax.sharding import PartitionSpec as P


F32 = jnp.float32
BF16 = jnp.bfloat16


def halves(table):
    high = table.astype(BF16)
    low = (table - high.astype(np.float64)).astype(BF16)
    return np.stack([high, low])


def dft(length, sign):
    index = np.arange(length)
    angle = 2.0 * np.pi * ((index[:, None] * index[None, :]) % length) / length
    cosine, sine = np.cos(angle), sign * np.sin(angle)
    return np.block([[cosine, -sine], [sine, cosine]])


def dft_halves(length, sign):
    outputs = np.arange(length).reshape(-1, 2).T
    parts = []
    for k in outputs:
        angle = 2.0 * np.pi * ((k[:, None] * np.arange(length // 2)[None, :]) % length) / length
        cosine, sine = np.cos(angle), sign * np.sin(angle)
        parts.append(np.block([[cosine, -sine], [sine, cosine]]))
    return parts


def dealt_rows(length, devices, swap):
    width = length // devices
    rows = []
    for s in range(devices):
        s = s ^ 1 if swap else s
        rows += [r * length + s * width + b for r in range(2) for b in range(width)]
    return np.array(rows)


def table_first(table, value):
    dot = functools.partial(jnp.dot, preferred_element_type=F32)
    high, low = split(value)
    m = table.shape[1]
    both = dot(jnp.concatenate([table[0], table[1]], axis=0), high)
    return both[:m] + (both[m:] + dot(table[0], low))


def table_last(value, table):
    dot = functools.partial(jnp.dot, preferred_element_type=F32)
    high, low = split(value)
    m = value.shape[0]
    both = dot(jnp.concatenate([high, low], axis=0), table[0])
    return both[:m] + (both[m:] + dot(high, table[1]))


def split(value):
    high = value.astype(BF16)
    return high, (value - high.astype(F32)).astype(BF16)


def collect_kernel(pieces, local, *rest):
    kept, done = rest[-1 - len(pieces) : -1], rest[-1]
    half = local.shape[0] // 2
    pool = lax.axis_index("pool")
    copies = [
        pltpu.make_async_copy(
            local.at[pl.ds(half * (1 - pool if other else pool) + start, count)], part, done.at[k]
        )
        for k, ((start, count, other), part) in enumerate(zip(pieces, kept))
    ]
    for copy in copies:
        copy.start()
    for copy in copies:
        copy.wait()


def transformed(x, wz, wy):
    n = x.shape[-1]
    rows = jnp.concatenate([x[:, 0].reshape(4 * n, n), x[:, 1].reshape(4 * n, n)], axis=1)
    y = table_last(rows, wz)
    mixed = []
    for k in range(2):
        first, second = y[2 * k * n : (2 * k + 1) * n], y[(2 * k + 1) * n : (2 * k + 2) * n]
        real = jnp.concatenate([first[:, :n], second[:, :n]], axis=1)
        imag = jnp.concatenate([first[:, n:], second[:, n:]], axis=1)
        mixed.append(table_first(wy[k], jnp.concatenate([real, imag], axis=0)).reshape(-1, 8, 2 * n))
    even, odd = mixed
    lower = lax.broadcasted_iota(jnp.int32, even.shape, 1) < 4
    return jnp.where(lower, even, odd), jnp.where(lower, odd, even)


def forward_first_kernel(own, arrived, wz, wy, tiles):
    n = own.shape[-1]
    step = pl.program_id(0)
    pair = pl.ds(2 * step, 2)
    for j, value in enumerate(transformed(own[pair] + arrived[pair], wz[...], wy[...])):
        for a in range(2):
            tiles[:, j, a, step] = value[:, :, a * n : (a + 1) * n]


def forward_second_kernel(own, arrived, wz, wy, tiles, spectrum, later, done):
    n = own.shape[-1]
    step = pl.program_id(0)
    last = pl.num_programs(0) - 1
    ready = tiles.shape[3]
    earlier = pltpu.make_async_copy(tiles, spectrum.at[:, :, :, pl.ds(0, ready)], done.at[0])

    @pl.when(step == 0)
    def _():
        earlier.start()

    pair = pl.ds(2 * step, 2)
    for j, value in enumerate(transformed(own[pair] + arrived[pair], wz[...], wy[...])):
        for a in range(2):
            later[step, :, j, a] = value[:, :, a * n : (a + 1) * n]

    sent = [
        pltpu.make_async_copy(later.at[i], spectrum.at[:, :, :, ready + i], done.at[1 + i])
        for i in range(spectrum.shape[3] - ready)
    ]
    for i, copy in enumerate(sent):

        @pl.when(step == i)
        def _(copy=copy):
            copy.start()

    @pl.when(step == last)
    def _():
        earlier.wait()
        for copy in sent:
            copy.wait()


def by_parts(table, even, odd):
    dot = functools.partial(jnp.dot, preferred_element_type=F32)
    (even_high, even_low), (odd_high, odd_low) = split(even), split(odd)
    main = [
        dot(jnp.concatenate([table[i, 0], table[i, 0]], axis=1), jnp.concatenate([high, low], axis=0))
        for i, (high, low) in enumerate(((even_high, even_low), (odd_high, odd_low)))
    ]
    zero = jnp.zeros(table.shape[2:], BF16)
    low = jnp.concatenate(
        [jnp.concatenate([table[0, 1], zero], axis=1), jnp.concatenate([zero, table[1, 1]], axis=1)], axis=0
    )
    return jnp.concatenate(main, axis=0) + dot(low, jnp.concatenate([even_high, odd_high], axis=0))


def middle_kernel(columns, wx, wxi, kernel, out, rows, back):
    n = kernel.shape[-1]
    length = kernel.shape[1]
    half = length // 2
    step = pl.program_id(0)
    for x in range(length):
        rows[pl.ds(PITCH * x, 8), :] = columns[x, step]
    grab = lambda j: rows[pl.ds(j, length, stride=PITCH), :]
    order = [(p, b) for p in range(2) for b in range(2)]
    fields = [jnp.concatenate([grab(4 * p + 2 * r + b) for p, b in order], axis=1) for r in range(2)]
    total = jnp.concatenate([f[:half] + f[half:] for f in fields], axis=0)
    difference = jnp.concatenate([f[:half] - f[half:] for f in fields], axis=0)
    spectrum = by_parts(wx, total, difference)
    both = jnp.concatenate([kernel[0], kernel[1]] * 2, axis=1)
    both = jnp.concatenate([both[:half], both[:half], both[half:], both[half:]], axis=0)
    spectrum = spectrum * both
    result = by_parts(wxi, spectrum[:length], spectrum[length:])
    even, odd = result[:length], result[length:]
    sides = (even + odd, even - odd)
    for i, (p, b) in enumerate(order):
        for r in range(2):
            for h, side in enumerate(sides):
                back[pl.ds(h * half * PITCH + 4 * p + 2 * r + b, half, stride=PITCH), :] = side[
                    r * half : (r + 1) * half, i * n : (i + 1) * n
                ]
    for x in range(length):
        out[x, step] = back[pl.ds(PITCH * x, 8), :]


def backward_kernel(start, columns, wyi, wzi, fxc, own, arrived, out):
    n = fxc.shape[-1]
    step = pl.program_id(0)
    place = start // 2 + step
    tiles = [jnp.concatenate([columns[:, j, a, place] for a in range(2)], axis=-1) for j in range(2)]
    lower = lax.broadcasted_iota(jnp.int32, tiles[0].shape, 1) < 4
    even = jnp.where(lower, tiles[0], tiles[1])
    odd = jnp.where(lower, tiles[1], tiles[0])
    rows = []
    for k, value in enumerate((even, odd)):
        y = table_first(wyi[k], value.reshape(2 * n, 2 * n))
        for a in range(2):
            rows.append(jnp.concatenate([y[:n, a * n : (a + 1) * n], y[n:, a * n : (a + 1) * n]], axis=1))
    x = table_last(jnp.concatenate(rows, axis=0), wzi[...])
    for k in range(2):
        for r in range(2):
            part = x[2 * k * n : (2 * k + 2) * n, r * n : (r + 1) * n].reshape(2, n, n)
            out[2 * step + k, r] = part + fxc[...] * (own[2 * step + k, r] + arrived[2 * step + k, r])


def place_kernel(pieces, slot, *rest):
    parts, out, done = rest[: len(pieces)], rest[-2], rest[-1]
    half = out.shape[0] // 2
    pool = lax.axis_index("pool")
    copies = []
    for (start, other), part in zip(pieces, parts):
        first = half * (1 - pool if other else pool) + start
        for k in range(part.shape[0]):
            copies.append(pltpu.make_async_copy(part.at[k], out.at[slot[first + k]], done.at[len(copies)]))
    for copy in copies:
        copy.start()
    for copy in copies:
        copy.wait()


def frequency(index, length):
    return ((index + length // 2) % length - length // 2).astype(F32)


def column_kernel(cutoff_mask, length):
    width = cutoff_mask.shape[1]
    start = lax.axis_index("slab") * width
    full_index = jnp.arange(length, dtype=jnp.int32)
    dealt_index = full_index.reshape(-1, 2).T.reshape(-1)
    part_index = start + jnp.arange(width, dtype=jnp.int32)
    first_square = frequency(dealt_index, length) ** 2
    part_square = frequency(part_index, length) ** 2
    last_square = frequency(full_index, length) ** 2
    total = part_square[:, None, None] + first_square[None, :, None] + last_square[None, None, :]
    unit = (2.0 * math.pi / length) ** 2
    mask = cutoff_mask.reshape(-1, 2, width, length).transpose(2, 1, 0, 3).reshape(width, length, length).astype(F32)
    scale = 1.0 / float(length) ** 3
    return (4.0 * math.pi * mask / (unit * total + 0.25)) * scale


RESIDENT = pl.BlockSpec(memory_space=pltpu.VMEM)
PITCH = 9


def taking(us):
    return pl.CostEstimate(flops=int(us * 1e8), bytes_accessed=0, transcendentals=0)


def per_device(drho_part, fxc, cutoff_mask, owner_table):
    local = drho_part[0]
    slots, _, planes, n, _ = local.shape
    devices = lax.axis_size("slab")
    mine = slots // 2
    tile = (2, planes, n, n)
    swap = [(0, 1), (1, 0)]
    limit = lambda share: pltpu.CompilerParams(vmem_limit_bytes=share << 20)
    ahead = [(0, mine // 2), (mine // 2, mine // 2)]
    behind = ahead

    forward = dft(n, -1.0)
    inverse = dft(n, 1.0)
    dealt = [dealt_rows(n, devices, s) for s in (False, True)]
    wz = jnp.asarray(halves(forward.T))
    wzi = jnp.asarray(halves(inverse.T))
    wy = jnp.asarray(np.stack([halves(forward[rows]) for rows in dealt]))
    wyi = jnp.asarray(np.stack([halves(inverse[:, rows]) for rows in dealt]))
    wx = jnp.asarray(np.stack([halves(w) for w in dft_halves(n, -1.0)]))
    wxi = jnp.asarray(np.stack([halves(w.T) for w in dft_halves(n, -1.0)]))

    far = pl.BlockSpec(memory_space=pl.ANY)
    scalars = pl.BlockSpec(memory_space=pltpu.SMEM)
    parts = lambda count: jax.ShapeDtypeStruct((count, *tile), F32)

    def collected(pieces, *earlier):
        return pl.pallas_call(
            functools.partial(collect_kernel, pieces),
            out_shape=tuple(parts(count) for _, count, _ in pieces),
            in_specs=[far] * (1 + len(earlier)),
            out_specs=(RESIDENT,) * len(pieces),
            scratch_shapes=[pltpu.SemaphoreType.DMA((len(pieces),))],
            compiler_params=limit(49),
            cost_estimate=taking(1),
        )(local, *earlier)

    (first,) = collected([(*ahead[0], True)])
    second, *own = collected([(*ahead[1], True), (*ahead[0], False), (*ahead[1], False)], first)
    arrived = []
    for sent in (first, second):
        arrived.append(lax.ppermute(sent, "pool", swap))

    shape = (devices // 2, 2, planes, mine // 2, 8, n)
    ready = ahead[0][1] // 2
    tiles = pl.pallas_call(
        forward_first_kernel,
        out_shape=jax.ShapeDtypeStruct((*shape[:3], ready, *shape[4:]), F32),
        grid=(ready,),
        in_specs=[RESIDENT] * 4,
        out_specs=RESIDENT,
        compiler_params=limit(40),
        cost_estimate=taking(2.4),
        name="forward0",
    )(own[0], arrived[0], wz, wy)
    later = shape[3] - ready
    spectrum = pl.pallas_call(
        forward_second_kernel,
        out_shape=jax.ShapeDtypeStruct(shape, F32),
        grid=(later,),
        in_specs=[RESIDENT] * 5,
        out_specs=far,
        scratch_shapes=[
            pltpu.VMEM((later, *shape[:3], *shape[4:]), F32),
            pltpu.SemaphoreType.DMA((1 + later,)),
        ],
        compiler_params=limit(40),
        cost_estimate=taking(2.4),
        name="forward1",
    )(own[1], arrived[1], wz, wy, tiles)

    kernel = column_kernel(cutoff_mask, n)
    index = jnp.arange(slots, dtype=jnp.int32)
    slot = jnp.sum(jnp.where(owner_table[None, :] == index[:, None], index[None, :], 0), axis=1)
    flat = (devices, planes * (mine // 2) * 8, n)
    columns = lax.all_to_all(spectrum.reshape(flat), "slab", split_axis=0, concat_axis=0, tiled=True)
    columns = columns.reshape(n, mine // 2, 8, n)
    columns = pl.pallas_call(
        middle_kernel,
        out_shape=jax.ShapeDtypeStruct(columns.shape, F32),
        grid=(mine // 2,),
        in_specs=[RESIDENT] * 4,
        out_specs=RESIDENT,
        scratch_shapes=[pltpu.VMEM((n * PITCH, n), F32)] * 2,
        compiler_params=limit(40),
        cost_estimate=taking(4),
        name="middle",
    )(columns, wx, wxi, kernel)
    columns = lax.all_to_all(columns.reshape(flat), "slab", split_axis=0, concat_axis=0, tiled=True)
    columns = columns.reshape(shape)

    results, others = [], []
    for start, count in behind:
        k = ahead.index((start, count))
        results.append(
            pl.pallas_call(
                functools.partial(backward_kernel, start),
                out_shape=parts(count),
                grid=(count // 2,),
                in_specs=[RESIDENT] * 6,
                out_specs=RESIDENT,
                compiler_params=limit(40),
                cost_estimate=taking(0.6 * count),
            )(columns, wyi, wzi, fxc, own[k], arrived[k])
        )
        others.append(lax.ppermute(results[-1], "pool", swap))

    def placed(pieces, arrays, out=None):
        aliases = {} if out is None else {1 + len(arrays): 0}
        kept = [] if out is None else [out]
        return pl.pallas_call(
            functools.partial(place_kernel, pieces),
            out_shape=jax.ShapeDtypeStruct(local.shape, F32),
            in_specs=[scalars] + [RESIDENT] * len(arrays) + [far] * len(kept),
            out_specs=far,
            scratch_shapes=[pltpu.SemaphoreType.DMA((sum(a.shape[0] for a in arrays),))],
            input_output_aliases=aliases,
            compiler_params=limit(40),
            cost_estimate=taking(1),
        )(slot, *arrays, *kept)

    starts = [start for start, _ in behind]
    out = placed([(start, False) for start in starts], results)
    return placed([(start, True) for start in starts], others, out)


def solution(mesh):
    placed = (
        P("pool", "group", None, "slab", None, None),
        P("slab", None, None),
        P(None, "slab", None),
        P("group"),
    )

    return jax.shard_map(
        per_device,
        mesh=mesh,
        in_specs=placed,
        out_specs=P("group", None, "slab", None, None),
        check_vma=False,
    )
```

```python
import functools
import math

import jax
import jax.numpy as jnp
import numpy as np
from jax import lax
from jax.experimental import pallas as pl
from jax.experimental.pallas import tpu as pltpu
from jax.sharding import PartitionSpec as P


F32 = jnp.float32
BF16 = jnp.bfloat16


def halves(table):
    high = table.astype(BF16)
    low = (table - high.astype(np.float64)).astype(BF16)
    return np.stack([high, low])


def dft(length, sign):
    index = np.arange(length)
    angle = 2.0 * np.pi * ((index[:, None] * index[None, :]) % length) / length
    cosine, sine = np.cos(angle), sign * np.sin(angle)
    return np.block([[cosine, -sine], [sine, cosine]])


def dft_halves(length, sign):
    outputs = np.arange(length).reshape(-1, 2).T
    parts = []
    for k in outputs:
        angle = 2.0 * np.pi * ((k[:, None] * np.arange(length // 2)[None, :]) % length) / length
        cosine, sine = np.cos(angle), sign * np.sin(angle)
        parts.append(np.block([[cosine, -sine], [sine, cosine]]))
    return parts


def dealt_rows(length, devices, swap):
    width = length // devices
    rows = []
    for s in range(devices):
        s = s ^ 1 if swap else s
        rows += [r * length + s * width + b for r in range(2) for b in range(width)]
    return np.array(rows)


def table_first(table, value):
    dot = functools.partial(jnp.dot, preferred_element_type=F32)
    high, low = split(value)
    m = table.shape[1]
    both = dot(jnp.concatenate([table[0], table[1]], axis=0), high)
    return both[:m] + (both[m:] + dot(table[0], low))


def table_last(value, table):
    dot = functools.partial(jnp.dot, preferred_element_type=F32)
    high, low = split(value)
    m = value.shape[0]
    both = dot(jnp.concatenate([high, low], axis=0), table[0])
    return both[:m] + (both[m:] + dot(high, table[1]))


def split(value):
    high = value.astype(BF16)
    return high, (value - high.astype(F32)).astype(BF16)


def collect_kernel(pieces, local, *rest):
    kept, done = rest[-1 - len(pieces) : -1], rest[-1]
    half = local.shape[0] // 2
    pool = lax.axis_index("pool")
    copies = [
        pltpu.make_async_copy(
            local.at[pl.ds(half * (1 - pool if other else pool) + start, count)], part, done.at[k]
        )
        for k, ((start, count, other), part) in enumerate(zip(pieces, kept))
    ]
    for copy in copies:
        copy.start()
    for copy in copies:
        copy.wait()


def transformed(x, wz, wy):
    n = x.shape[-1]
    rows = jnp.concatenate([x[:, 0].reshape(4 * n, n), x[:, 1].reshape(4 * n, n)], axis=1)
    y = table_last(rows, wz)
    mixed = []
    for k in range(2):
        first, second = y[2 * k * n : (2 * k + 1) * n], y[(2 * k + 1) * n : (2 * k + 2) * n]
        real = jnp.concatenate([first[:, :n], second[:, :n]], axis=1)
        imag = jnp.concatenate([first[:, n:], second[:, n:]], axis=1)
        mixed.append(table_first(wy[k], jnp.concatenate([real, imag], axis=0)).reshape(-1, 8, 2 * n))
    even, odd = mixed
    lower = lax.broadcasted_iota(jnp.int32, even.shape, 1) < 4
    return jnp.where(lower, even, odd), jnp.where(lower, odd, even)


def forward_first_kernel(start, own, arrived, wz, wy, local, tiles, own_next, done):
    n = own.shape[-1]
    step = pl.program_id(0)
    first = local.shape[0] // 2 * lax.axis_index("pool") + start
    fetch = pltpu.make_async_copy(local.at[pl.ds(first, own_next.shape[0])], own_next, done)

    @pl.when(step == 0)
    def _():
        fetch.start()

    pair = pl.ds(2 * step, 2)
    for j, value in enumerate(transformed(own[pair] + arrived[pair], wz[...], wy[...])):
        for a in range(2):
            tiles[:, j, a, step] = value[:, :, a * n : (a + 1) * n]

    @pl.when(step == pl.num_programs(0) - 1)
    def _():
        fetch.wait()


def forward_second_kernel(own, arrived, wz, wy, tiles, spectrum, later, done):
    n = own.shape[-1]
    step = pl.program_id(0)
    last = pl.num_programs(0) - 1
    ready = tiles.shape[3]
    earlier = pltpu.make_async_copy(tiles, spectrum.at[:, :, :, pl.ds(0, ready)], done.at[0])

    @pl.when(step == 0)
    def _():
        earlier.start()

    pair = pl.ds(2 * step, 2)
    for j, value in enumerate(transformed(own[pair] + arrived[pair], wz[...], wy[...])):
        for a in range(2):
            later[step, :, j, a] = value[:, :, a * n : (a + 1) * n]

    sent = [
        pltpu.make_async_copy(later.at[i], spectrum.at[:, :, :, ready + i], done.at[1 + i])
        for i in range(spectrum.shape[3] - ready)
    ]
    for i, copy in enumerate(sent):

        @pl.when(step == i)
        def _(copy=copy):
            copy.start()

    @pl.when(step == last)
    def _():
        earlier.wait()
        for copy in sent:
            copy.wait()


def by_parts(table, even, odd):
    dot = functools.partial(jnp.dot, preferred_element_type=F32)
    (even_high, even_low), (odd_high, odd_low) = split(even), split(odd)
    main = [
        dot(jnp.concatenate([table[i, 0], table[i, 0]], axis=1), jnp.concatenate([high, low], axis=0))
        for i, (high, low) in enumerate(((even_high, even_low), (odd_high, odd_low)))
    ]
    zero = jnp.zeros(table.shape[2:], BF16)
    low = jnp.concatenate(
        [jnp.concatenate([table[0, 1], zero], axis=1), jnp.concatenate([zero, table[1, 1]], axis=1)], axis=0
    )
    return jnp.concatenate(main, axis=0) + dot(low, jnp.concatenate([even_high, odd_high], axis=0))


def middle_kernel(columns, wx, wxi, kernel, out, rows, back):
    n = kernel.shape[-1]
    length = kernel.shape[1]
    half = length // 2
    step = pl.program_id(0)
    pairs = rows.shape[0]
    for m in range(pairs):
        for x in range(length):
            rows[m, pl.ds(PITCH * x, 8), :] = columns[x, pairs * step + m]
    order = [(m, p, b) for m in range(pairs) for p in range(2) for b in range(2)]
    grab = lambda m, j: rows[m, pl.ds(j, length, stride=PITCH), :]
    fields = [jnp.concatenate([grab(m, 4 * p + 2 * r + b) for m, p, b in order], axis=1) for r in range(2)]
    total = jnp.concatenate([f[:half] + f[half:] for f in fields], axis=0)
    difference = jnp.concatenate([f[:half] - f[half:] for f in fields], axis=0)
    spectrum = by_parts(wx, total, difference)
    both = jnp.concatenate([kernel[0], kernel[1]] * (2 * pairs), axis=1)
    both = jnp.concatenate([both[:half], both[:half], both[half:], both[half:]], axis=0)
    spectrum = spectrum * both
    result = by_parts(wxi, spectrum[:length], spectrum[length:])
    even, odd = result[:length], result[length:]
    sides = (even + odd, even - odd)
    for i, (m, p, b) in enumerate(order):
        for r in range(2):
            for h, side in enumerate(sides):
                back[m, pl.ds(h * half * PITCH + 4 * p + 2 * r + b, half, stride=PITCH), :] = side[
                    r * half : (r + 1) * half, i * n : (i + 1) * n
                ]
    for m in range(pairs):
        for x in range(length):
            out[x, pairs * step + m] = back[m, pl.ds(PITCH * x, 8), :]


def backward_kernel(start, columns, wyi, wzi, fxc, own, arrived, out):
    n = fxc.shape[-1]
    step = pl.program_id(0)
    place = start // 2 + step
    tiles = [jnp.concatenate([columns[:, j, a, place] for a in range(2)], axis=-1) for j in range(2)]
    lower = lax.broadcasted_iota(jnp.int32, tiles[0].shape, 1) < 4
    even = jnp.where(lower, tiles[0], tiles[1])
    odd = jnp.where(lower, tiles[1], tiles[0])
    rows = []
    for k, value in enumerate((even, odd)):
        y = table_first(wyi[k], value.reshape(2 * n, 2 * n))
        for a in range(2):
            rows.append(jnp.concatenate([y[:n, a * n : (a + 1) * n], y[n:, a * n : (a + 1) * n]], axis=1))
    x = table_last(jnp.concatenate(rows, axis=0), wzi[...])
    for k in range(2):
        for r in range(2):
            part = x[2 * k * n : (2 * k + 2) * n, r * n : (r + 1) * n].reshape(2, n, n)
            out[2 * step + k, r] = part + fxc[...] * (own[2 * step + k, r] + arrived[2 * step + k, r])


def place_kernel(pieces, slot, *rest):
    parts, out, done = rest[: len(pieces)], rest[-2], rest[-1]
    half = out.shape[0] // 2
    pool = lax.axis_index("pool")
    copies = []
    for (start, other), part in zip(pieces, parts):
        first = half * (1 - pool if other else pool) + start
        for k in range(part.shape[0]):
            copies.append(pltpu.make_async_copy(part.at[k], out.at[slot[first + k]], done.at[len(copies)]))
    for copy in copies:
        copy.start()
    for copy in copies:
        copy.wait()


def frequency(index, length):
    return ((index + length // 2) % length - length // 2).astype(F32)


def column_kernel(cutoff_mask, length):
    width = cutoff_mask.shape[1]
    start = lax.axis_index("slab") * width
    full_index = jnp.arange(length, dtype=jnp.int32)
    dealt_index = full_index.reshape(-1, 2).T.reshape(-1)
    part_index = start + jnp.arange(width, dtype=jnp.int32)
    first_square = frequency(dealt_index, length) ** 2
    part_square = frequency(part_index, length) ** 2
    last_square = frequency(full_index, length) ** 2
    total = part_square[:, None, None] + first_square[None, :, None] + last_square[None, None, :]
    unit = (2.0 * math.pi / length) ** 2
    mask = cutoff_mask.reshape(-1, 2, width, length).transpose(2, 1, 0, 3).reshape(width, length, length).astype(F32)
    scale = 1.0 / float(length) ** 3
    return (4.0 * math.pi * mask / (unit * total + 0.25)) * scale


RESIDENT = pl.BlockSpec(memory_space=pltpu.VMEM)
PITCH = 9


def taking(us):
    return pl.CostEstimate(flops=int(us * 1e8), bytes_accessed=0, transcendentals=0)


def per_device(drho_part, fxc, cutoff_mask, owner_table):
    local = drho_part[0]
    slots, _, planes, n, _ = local.shape
    devices = lax.axis_size("slab")
    mine = slots // 2
    tile = (2, planes, n, n)
    swap = [(0, 1), (1, 0)]
    limit = lambda share: pltpu.CompilerParams(vmem_limit_bytes=share << 20)
    ahead = [(0, mine // 2), (mine // 2, mine // 2)]
    behind = ahead

    forward = dft(n, -1.0)
    inverse = dft(n, 1.0)
    dealt = [dealt_rows(n, devices, s) for s in (False, True)]
    wz = jnp.asarray(halves(forward.T))
    wzi = jnp.asarray(halves(inverse.T))
    wy = jnp.asarray(np.stack([halves(forward[rows]) for rows in dealt]))
    wyi = jnp.asarray(np.stack([halves(inverse[:, rows]) for rows in dealt]))
    wx = jnp.asarray(np.stack([halves(w) for w in dft_halves(n, -1.0)]))
    wxi = jnp.asarray(np.stack([halves(w.T) for w in dft_halves(n, -1.0)]))

    far = pl.BlockSpec(memory_space=pl.ANY)
    scalars = pl.BlockSpec(memory_space=pltpu.SMEM)
    parts = lambda count: jax.ShapeDtypeStruct((count, *tile), F32)

    def collected(pieces, *earlier):
        return pl.pallas_call(
            functools.partial(collect_kernel, pieces),
            out_shape=tuple(parts(count) for _, count, _ in pieces),
            in_specs=[far] * (1 + len(earlier)),
            out_specs=(RESIDENT,) * len(pieces),
            scratch_shapes=[pltpu.SemaphoreType.DMA((len(pieces),))],
            compiler_params=limit(49),
            cost_estimate=taking(1),
        )(local, *earlier)

    (first,) = collected([(*ahead[0], True)])
    second, own_first = collected([(*ahead[1], True), (*ahead[0], False)], first)
    arrived = []
    for sent in (first, second):
        arrived.append(lax.ppermute(sent, "pool", swap))

    shape = (devices // 2, 2, planes, mine // 2, 8, n)
    ready = ahead[0][1] // 2
    tiles, own_second = pl.pallas_call(
        functools.partial(forward_first_kernel, ahead[1][0]),
        out_shape=(jax.ShapeDtypeStruct((*shape[:3], ready, *shape[4:]), F32), parts(ahead[1][1])),
        grid=(ready,),
        in_specs=[RESIDENT] * 4 + [far],
        out_specs=(RESIDENT, RESIDENT),
        scratch_shapes=[pltpu.SemaphoreType.DMA],
        compiler_params=limit(49),
        cost_estimate=taking(2.4),
        name="forward0",
    )(own_first, arrived[0], wz, wy, local)
    own = [own_first, own_second]
    later = shape[3] - ready
    spectrum = pl.pallas_call(
        forward_second_kernel,
        out_shape=jax.ShapeDtypeStruct(shape, F32),
        grid=(later,),
        in_specs=[RESIDENT] * 5,
        out_specs=far,
        scratch_shapes=[
            pltpu.VMEM((later, *shape[:3], *shape[4:]), F32),
            pltpu.SemaphoreType.DMA((1 + later,)),
        ],
        compiler_params=limit(40),
        cost_estimate=taking(2.4),
        name="forward1",
    )(own[1], arrived[1], wz, wy, tiles)

    kernel = column_kernel(cutoff_mask, n)
    index = jnp.arange(slots, dtype=jnp.int32)
    slot = jnp.sum(jnp.where(owner_table[None, :] == index[:, None], index[None, :], 0), axis=1)
    flat = (devices, planes * (mine // 2) * 8, n)
    columns = lax.all_to_all(spectrum.reshape(flat), "slab", split_axis=0, concat_axis=0, tiled=True)
    columns = columns.reshape(n, mine // 2, 8, n)
    columns = pl.pallas_call(
        middle_kernel,
        out_shape=jax.ShapeDtypeStruct(columns.shape, F32),
        grid=(mine // 4,),
        in_specs=[RESIDENT] * 4,
        out_specs=RESIDENT,
        scratch_shapes=[pltpu.VMEM((2, n * PITCH, n), F32)] * 2,
        compiler_params=limit(40),
        cost_estimate=taking(4),
        name="middle",
    )(columns, wx, wxi, kernel)
    columns = lax.all_to_all(columns.reshape(flat), "slab", split_axis=0, concat_axis=0, tiled=True)
    columns = columns.reshape(shape)

    results, others = [], []
    for start, count in behind:
        k = ahead.index((start, count))
        results.append(
            pl.pallas_call(
                functools.partial(backward_kernel, start),
                out_shape=parts(count),
                grid=(count // 2,),
                in_specs=[RESIDENT] * 6,
                out_specs=RESIDENT,
                compiler_params=limit(40),
                cost_estimate=taking(0.6 * count),
            )(columns, wyi, wzi, fxc, own[k], arrived[k])
        )
        others.append(lax.ppermute(results[-1], "pool", swap))

    def placed(pieces, arrays, out=None):
        aliases = {} if out is None else {1 + len(arrays): 0}
        kept = [] if out is None else [out]
        return pl.pallas_call(
            functools.partial(place_kernel, pieces),
            out_shape=jax.ShapeDtypeStruct(local.shape, F32),
            in_specs=[scalars] + [RESIDENT] * len(arrays) + [far] * len(kept),
            out_specs=far,
            scratch_shapes=[pltpu.SemaphoreType.DMA((sum(a.shape[0] for a in arrays),))],
            input_output_aliases=aliases,
            compiler_params=limit(40),
            cost_estimate=taking(1),
        )(slot, *arrays, *kept)

    starts = [start for start, _ in behind]
    out = placed([(start, False) for start in starts], results)
    return placed([(start, True) for start in starts], others, out)


def solution(mesh):
    placed = (
        P("pool", "group", None, "slab", None, None),
        P("slab", None, None),
        P(None, "slab", None),
        P("group"),
    )

    return jax.shard_map(
        per_device,
        mesh=mesh,
        in_specs=placed,
        out_specs=P("group", None, "slab", None, None),
        check_vma=False,
    )
```

```python
import functools
import math

import jax
import jax.numpy as jnp
import numpy as np
from jax import lax
from jax.experimental import pallas as pl
from jax.experimental.pallas import tpu as pltpu
from jax.sharding import PartitionSpec as P


F32 = jnp.float32
BF16 = jnp.bfloat16


def halves(table):
    high = table.astype(BF16)
    low = (table - high.astype(np.float64)).astype(BF16)
    return np.stack([high, low])


def dft(length, sign):
    index = np.arange(length)
    angle = 2.0 * np.pi * ((index[:, None] * index[None, :]) % length) / length
    cosine, sine = np.cos(angle), sign * np.sin(angle)
    return np.block([[cosine, -sine], [sine, cosine]])


def dft_halves(length, sign):
    outputs = np.arange(length).reshape(-1, 2).T
    parts = []
    for k in outputs:
        angle = 2.0 * np.pi * ((k[:, None] * np.arange(length // 2)[None, :]) % length) / length
        cosine, sine = np.cos(angle), sign * np.sin(angle)
        parts.append(np.block([[cosine, -sine], [sine, cosine]]))
    return parts


def dealt_rows(length, devices, swap):
    width = length // devices
    rows = []
    for s in range(devices):
        s = s ^ 1 if swap else s
        rows += [r * length + s * width + b for r in range(2) for b in range(width)]
    return np.array(rows)


def table_first(table, value):
    dot = functools.partial(jnp.dot, preferred_element_type=F32)
    high, low = split(value)
    m = table.shape[1]
    both = dot(jnp.concatenate([table[0], table[1]], axis=0), high)
    return both[:m] + (both[m:] + dot(table[0], low))


def table_last(value, table):
    dot = functools.partial(jnp.dot, preferred_element_type=F32)
    high, low = split(value)
    m = value.shape[0]
    both = dot(jnp.concatenate([high, low], axis=0), table[0])
    return both[:m] + (both[m:] + dot(high, table[1]))


def split(value):
    high = value.astype(BF16)
    return high, (value - high.astype(F32)).astype(BF16)


def collect_kernel(pieces, local, *rest):
    kept, done = rest[-1 - len(pieces) : -1], rest[-1]
    half = local.shape[0] // 2
    pool = lax.axis_index("pool")
    copies = [
        pltpu.make_async_copy(
            local.at[pl.ds(half * (1 - pool if other else pool) + start, count)], part, done.at[k]
        )
        for k, ((start, count, other), part) in enumerate(zip(pieces, kept))
    ]
    for copy in copies:
        copy.start()
    for copy in copies:
        copy.wait()


def transformed(x, wz, wy):
    n = x.shape[-1]
    rows = jnp.concatenate([x[:, 0].reshape(4 * n, n), x[:, 1].reshape(4 * n, n)], axis=1)
    y = table_last(rows, wz)
    mixed = []
    for k in range(2):
        first, second = y[2 * k * n : (2 * k + 1) * n], y[(2 * k + 1) * n : (2 * k + 2) * n]
        real = jnp.concatenate([first[:, :n], second[:, :n]], axis=1)
        imag = jnp.concatenate([first[:, n:], second[:, n:]], axis=1)
        mixed.append(table_first(wy[k], jnp.concatenate([real, imag], axis=0)).reshape(-1, 8, 2 * n))
    even, odd = mixed
    lower = lax.broadcasted_iota(jnp.int32, even.shape, 1) < 4
    return jnp.where(lower, even, odd), jnp.where(lower, odd, even)


def forward_first_kernel(start, own, arrived, wz, wy, local, tiles, own_next, done):
    n = own.shape[-1]
    step = pl.program_id(0)
    first = local.shape[0] // 2 * lax.axis_index("pool") + start
    fetch = pltpu.make_async_copy(local.at[pl.ds(first, own_next.shape[0])], own_next, done)

    @pl.when(step == 0)
    def _():
        fetch.start()

    pair = pl.ds(2 * step, 2)
    for j, value in enumerate(transformed(own[pair] + arrived[pair], wz[...], wy[...])):
        for a in range(2):
            tiles[:, j, a, step] = value[:, :, a * n : (a + 1) * n]

    @pl.when(step == pl.num_programs(0) - 1)
    def _():
        fetch.wait()


def forward_second_kernel(own, arrived, wz, wy, tiles, spectrum, later, done):
    n = own.shape[-1]
    step = pl.program_id(0)
    last = pl.num_programs(0) - 1
    ready = tiles.shape[3]
    earlier = pltpu.make_async_copy(tiles, spectrum.at[:, :, :, pl.ds(0, ready)], done.at[0])

    @pl.when(step == 0)
    def _():
        earlier.start()

    pair = pl.ds(2 * step, 2)
    for j, value in enumerate(transformed(own[pair] + arrived[pair], wz[...], wy[...])):
        for a in range(2):
            later[step, :, j, a] = value[:, :, a * n : (a + 1) * n]

    sent = [
        pltpu.make_async_copy(later.at[i], spectrum.at[:, :, :, ready + i], done.at[1 + i])
        for i in range(spectrum.shape[3] - ready)
    ]
    for i, copy in enumerate(sent):

        @pl.when(step == i)
        def _(copy=copy):
            copy.start()

    @pl.when(step == last)
    def _():
        earlier.wait()
        for copy in sent:
            copy.wait()


def by_parts(table, even, odd):
    dot = functools.partial(jnp.dot, preferred_element_type=F32)
    (even_high, even_low), (odd_high, odd_low) = split(even), split(odd)
    main = [
        dot(jnp.concatenate([table[i, 0], table[i, 0]], axis=1), jnp.concatenate([high, low], axis=0))
        for i, (high, low) in enumerate(((even_high, even_low), (odd_high, odd_low)))
    ]
    zero = jnp.zeros(table.shape[2:], BF16)
    low = jnp.concatenate(
        [jnp.concatenate([table[0, 1], zero], axis=1), jnp.concatenate([zero, table[1, 1]], axis=1)], axis=0
    )
    return jnp.concatenate(main, axis=0) + dot(low, jnp.concatenate([even_high, odd_high], axis=0))


def middle_kernel(columns, wx, wxi, kernel, out, rows, back):
    n = kernel.shape[-1]
    length = kernel.shape[1]
    half = length // 2
    step = pl.program_id(0)
    pairs = rows.shape[0]
    for m in range(pairs):
        for x in range(length):
            rows[m, pl.ds(PITCH * x, 8), :] = columns[x, pairs * step + m]
    order = [(m, p, b) for m in range(pairs) for p in range(2) for b in range(2)]
    grab = lambda m, j: rows[m, pl.ds(j, length, stride=PITCH), :]
    fields = [jnp.concatenate([grab(m, 4 * p + 2 * r + b) for m, p, b in order], axis=1) for r in range(2)]
    total = jnp.concatenate([f[:half] + f[half:] for f in fields], axis=0)
    difference = jnp.concatenate([f[:half] - f[half:] for f in fields], axis=0)
    spectrum = by_parts(wx, total, difference)
    both = jnp.concatenate([kernel[0], kernel[1]] * (2 * pairs), axis=1)
    both = jnp.concatenate([both[:half], both[:half], both[half:], both[half:]], axis=0)
    spectrum = spectrum * both
    result = by_parts(wxi, spectrum[:length], spectrum[length:])
    even, odd = result[:length], result[length:]
    sides = (even + odd, even - odd)
    for i, (m, p, b) in enumerate(order):
        for r in range(2):
            for h, side in enumerate(sides):
                back[m, pl.ds(h * half * PITCH + 4 * p + 2 * r + b, half, stride=PITCH), :] = side[
                    r * half : (r + 1) * half, i * n : (i + 1) * n
                ]
    for m in range(pairs):
        for x in range(length):
            out[x, pairs * step + m] = back[m, pl.ds(PITCH * x, 8), :]


def backward_pair(start, step, columns, wyi, wzi, fxc, own, arrived, out):
    n = fxc.shape[-1]
    place = start // 2 + step
    tiles = [jnp.concatenate([columns[:, j, a, place] for a in range(2)], axis=-1) for j in range(2)]
    lower = lax.broadcasted_iota(jnp.int32, tiles[0].shape, 1) < 4
    even = jnp.where(lower, tiles[0], tiles[1])
    odd = jnp.where(lower, tiles[1], tiles[0])
    rows = []
    for k, value in enumerate((even, odd)):
        y = table_first(wyi[k], value.reshape(2 * n, 2 * n))
        for a in range(2):
            rows.append(jnp.concatenate([y[:n, a * n : (a + 1) * n], y[n:, a * n : (a + 1) * n]], axis=1))
    x = table_last(jnp.concatenate(rows, axis=0), wzi[...])
    for k in range(2):
        for r in range(2):
            part = x[2 * k * n : (2 * k + 2) * n, r * n : (r + 1) * n].reshape(2, n, n)
            out[2 * step + k, r] = part + fxc[...] * (own[2 * step + k, r] + arrived[2 * step + k, r])


def backward_kernel(start, *refs):
    for step in range(refs[-1].shape[0] // 2):
        backward_pair(start, step, *refs)


def place_kernel(pieces, slot, *rest):
    parts, out, done = rest[: len(pieces)], rest[-2], rest[-1]
    half = out.shape[0] // 2
    pool = lax.axis_index("pool")
    copies = []
    for (start, other), part in zip(pieces, parts):
        first = half * (1 - pool if other else pool) + start
        for k in range(part.shape[0]):
            copies.append(pltpu.make_async_copy(part.at[k], out.at[slot[first + k]], done.at[len(copies)]))
    for copy in copies:
        copy.start()
    for copy in copies:
        copy.wait()


def frequency(index, length):
    return ((index + length // 2) % length - length // 2).astype(F32)


def column_kernel(cutoff_mask, length):
    width = cutoff_mask.shape[1]
    start = lax.axis_index("slab") * width
    full_index = jnp.arange(length, dtype=jnp.int32)
    dealt_index = full_index.reshape(-1, 2).T.reshape(-1)
    part_index = start + jnp.arange(width, dtype=jnp.int32)
    first_square = frequency(dealt_index, length) ** 2
    part_square = frequency(part_index, length) ** 2
    last_square = frequency(full_index, length) ** 2
    total = part_square[:, None, None] + first_square[None, :, None] + last_square[None, None, :]
    unit = (2.0 * math.pi / length) ** 2
    mask = cutoff_mask.reshape(-1, 2, width, length).transpose(2, 1, 0, 3).reshape(width, length, length).astype(F32)
    scale = 1.0 / float(length) ** 3
    return (4.0 * math.pi * mask / (unit * total + 0.25)) * scale


RESIDENT = pl.BlockSpec(memory_space=pltpu.VMEM)
PITCH = 9


def taking(us):
    return pl.CostEstimate(flops=int(us * 1e8), bytes_accessed=0, transcendentals=0)


def per_device(drho_part, fxc, cutoff_mask, owner_table):
    local = drho_part[0]
    slots, _, planes, n, _ = local.shape
    devices = lax.axis_size("slab")
    mine = slots // 2
    tile = (2, planes, n, n)
    swap = [(0, 1), (1, 0)]
    limit = lambda share: pltpu.CompilerParams(vmem_limit_bytes=share << 20)
    ahead = [(0, mine // 2), (mine // 2, mine // 2)]
    behind = ahead

    forward = dft(n, -1.0)
    inverse = dft(n, 1.0)
    dealt = [dealt_rows(n, devices, s) for s in (False, True)]
    wz = jnp.asarray(halves(forward.T))
    wzi = jnp.asarray(halves(inverse.T))
    wy = jnp.asarray(np.stack([halves(forward[rows]) for rows in dealt]))
    wyi = jnp.asarray(np.stack([halves(inverse[:, rows]) for rows in dealt]))
    wx = jnp.asarray(np.stack([halves(w) for w in dft_halves(n, -1.0)]))
    wxi = jnp.asarray(np.stack([halves(w.T) for w in dft_halves(n, -1.0)]))

    far = pl.BlockSpec(memory_space=pl.ANY)
    scalars = pl.BlockSpec(memory_space=pltpu.SMEM)
    parts = lambda count: jax.ShapeDtypeStruct((count, *tile), F32)

    def collected(pieces, *earlier):
        return pl.pallas_call(
            functools.partial(collect_kernel, pieces),
            out_shape=tuple(parts(count) for _, count, _ in pieces),
            in_specs=[far] * (1 + len(earlier)),
            out_specs=(RESIDENT,) * len(pieces),
            scratch_shapes=[pltpu.SemaphoreType.DMA((len(pieces),))],
            compiler_params=limit(49),
            cost_estimate=taking(1),
        )(local, *earlier)

    (first,) = collected([(*ahead[0], True)])
    second, own_first = collected([(*ahead[1], True), (*ahead[0], False)], first)
    arrived = []
    for sent in (first, second):
        arrived.append(lax.ppermute(sent, "pool", swap))

    shape = (devices // 2, 2, planes, mine // 2, 8, n)
    ready = ahead[0][1] // 2
    tiles, own_second = pl.pallas_call(
        functools.partial(forward_first_kernel, ahead[1][0]),
        out_shape=(jax.ShapeDtypeStruct((*shape[:3], ready, *shape[4:]), F32), parts(ahead[1][1])),
        grid=(ready,),
        in_specs=[RESIDENT] * 4 + [far],
        out_specs=(RESIDENT, RESIDENT),
        scratch_shapes=[pltpu.SemaphoreType.DMA],
        compiler_params=limit(49),
        cost_estimate=taking(2.4),
        name="forward0",
    )(own_first, arrived[0], wz, wy, local)
    own = [own_first, own_second]
    later = shape[3] - ready
    spectrum = pl.pallas_call(
        forward_second_kernel,
        out_shape=jax.ShapeDtypeStruct(shape, F32),
        grid=(later,),
        in_specs=[RESIDENT] * 5,
        out_specs=far,
        scratch_shapes=[
            pltpu.VMEM((later, *shape[:3], *shape[4:]), F32),
            pltpu.SemaphoreType.DMA((1 + later,)),
        ],
        compiler_params=limit(40),
        cost_estimate=taking(2.4),
        name="forward1",
    )(own[1], arrived[1], wz, wy, tiles)

    kernel = column_kernel(cutoff_mask, n)
    index = jnp.arange(slots, dtype=jnp.int32)
    slot = jnp.sum(jnp.where(owner_table[None, :] == index[:, None], index[None, :], 0), axis=1)
    flat = (devices, planes * (mine // 2) * 8, n)
    columns = lax.all_to_all(spectrum.reshape(flat), "slab", split_axis=0, concat_axis=0, tiled=True)
    columns = columns.reshape(n, mine // 2, 8, n)
    columns = pl.pallas_call(
        middle_kernel,
        out_shape=jax.ShapeDtypeStruct(columns.shape, F32),
        grid=(1,),
        in_specs=[RESIDENT] * 4,
        out_specs=RESIDENT,
        scratch_shapes=[pltpu.VMEM((mine // 2, n * PITCH, n), F32)] * 2,
        compiler_params=limit(40),
        cost_estimate=taking(4),
        name="middle",
    )(columns, wx, wxi, kernel)
    columns = lax.all_to_all(columns.reshape(flat), "slab", split_axis=0, concat_axis=0, tiled=True)
    columns = columns.reshape(shape)

    results, others = [], []
    for start, count in behind:
        k = ahead.index((start, count))
        results.append(
            pl.pallas_call(
                functools.partial(backward_kernel, start),
                out_shape=parts(count),
                grid=(1,),
                in_specs=[RESIDENT] * 6,
                out_specs=RESIDENT,
                compiler_params=limit(40),
                cost_estimate=taking(0.6 * count),
            )(columns, wyi, wzi, fxc, own[k], arrived[k])
        )
        others.append(lax.ppermute(results[-1], "pool", swap))

    def placed(pieces, arrays, out=None):
        aliases = {} if out is None else {1 + len(arrays): 0}
        kept = [] if out is None else [out]
        return pl.pallas_call(
            functools.partial(place_kernel, pieces),
            out_shape=jax.ShapeDtypeStruct(local.shape, F32),
            in_specs=[scalars] + [RESIDENT] * len(arrays) + [far] * len(kept),
            out_specs=far,
            scratch_shapes=[pltpu.SemaphoreType.DMA((sum(a.shape[0] for a in arrays),))],
            input_output_aliases=aliases,
            compiler_params=limit(40),
            cost_estimate=taking(1),
        )(slot, *arrays, *kept)

    starts = [start for start, _ in behind]
    out = placed([(start, False) for start in starts], results)
    return placed([(start, True) for start in starts], others, out)


def solution(mesh):
    placed = (
        P("pool", "group", None, "slab", None, None),
        P("slab", None, None),
        P(None, "slab", None),
        P("group"),
    )

    return jax.shard_map(
        per_device,
        mesh=mesh,
        in_specs=placed,
        out_specs=P("group", None, "slab", None, None),
        check_vma=False,
    )
```
